128 devices in a mesh: batch: 8 (over y, core), vocab: 16 (over x, z).
Axes of the slice: x: 4, y: 4, z: 4, core: 2. Of those that a mesh axis runs over, the one named last changes fastest.
Arguments:
- hidden: bfloat16 [65536, 768], P(('batch', 'vocab')), may hold values from -150 to 150, as said below
- dense_w: bfloat16 [768, 768], replicated, may hold values from -0.21875 to 0.21875
- dense_b: float32 [768], replicated, may hold values from -3 to 3
- norm_gain: float32 [768], replicated, may hold values from 0.5 to 1.5
- norm_bias: float32 [768], replicated, may hold values from -2 to 2
- vocabulary_weight: bfloat16 [768, 30720], P(None, 'vocab'), may hold values from -0.21875 to 0.21875
- vocabulary_bias: bfloat16 [30720], P('vocab'), may hold values from -5 to 5
- lengths: int32 [256], P('batch'), may hold values from 32 to 256
- term_ids: int32 [256, 128], P('batch'), may hold values from -1 to 30521, as said below
Outputs:
- vectors: float32 [256, 30720], P('batch', 'vocab')
- posting_weights: float32 [128, 5, 128], P(('batch', 'vocab'))
- posting_key_codes: int32 [128, 5, 128], P(('batch', 'vocab'))
The draws below stay inside these ranges and needn't reach their ends.
Inputs may be any that keep to these rules, and one draw needn't show every extreme that they name: `hidden`: the last encoder layer's states. `term_ids`: no term appears twice in one passage and every term is below 30522. Within the 32 passages of one batch shard, the terms t with one value of t // 1920 and one value of t % (128) number at most 5, and in every draw one owner t % (128) reaches 5 for every batch shard and every value of t // 1920.
All inputs are finite; a program needn't handle non-finite values.
Results may differ from the reference program's by a relative error of at most 0.0009.
Values may be sent and summed in bfloat16 or wider, within the bound.
A program may use at most 64 MiB of HBM per device.

```python
import jax
import jax.numpy as jnp
from jax import lax

MODEL_WIDTH = 768
VOCAB = 30522
VOCAB_PADDED = 30720
L = 256
K = 128
PB = 32
PAS = 256
TOKENS = 65536
POSTING_LIMIT = 5
N_BATCH = 8
N_VOCAB = 16


def draw_hidden(key, part):
    streams = jax.random.split(jax.random.fold_in(key, 5), 3)
    row_scales = jnp.exp(jax.random.uniform(streams[1], (TOKENS, 1), jnp.float32, jnp.log(0.5), jnp.log(5.0)))
    column_scales = jnp.exp(jax.random.uniform(streams[2], (1, MODEL_WIDTH), jnp.float32, jnp.log(0.5), jnp.log(5.0)))
    basic = jax.random.normal(streams[0], (TOKENS, MODEL_WIDTH), jnp.float32)
    basic = jnp.clip(basic, -6.0, 6.0)
    return (basic * row_scales * column_scales).astype(jnp.bfloat16)


def shard_terms(shard_key, hot_owner, boosts):
    device_list = N_BATCH * N_VOCAB
    owner_extent = VOCAB_PADDED // N_VOCAB // device_list
    cells = N_VOCAB * device_list
    total = cells * POSTING_LIMIT
    streams = jax.random.split(shard_key, 4)
    entries = jnp.arange(total, dtype=jnp.int32)
    cell_index = entries // POSTING_LIMIT
    copy_index = entries % POSTING_LIMIT
    vocab_shard = cell_index // device_list
    owners = cell_index % device_list
    jitter = jax.random.randint(streams[0], (total,), 0, 1024)
    offsets = jax.random.randint(streams[1], (cells,), 0, owner_extent)
    limits = jnp.minimum(owner_extent, (VOCAB - owners - vocab_shard * owner_extent * device_list + device_list - 1) // device_list)
    residue = (offsets[cell_index] + copy_index) % limits
    terms = (vocab_shard * owner_extent + residue) * device_list + owners
    drawn = jitter + boosts[owners] + 2048 - jnp.minimum(copy_index * 300, 2047)
    scores = jnp.where(owners == hot_owner, 3584 + jitter, drawn) * 32768 + entries
    chosen = lax.top_k(scores, PB * K)[1]
    kept = jax.random.randint(streams[2], (), PB * K * 3 // 4, PB * K + 1)
    ranked = jnp.where(jnp.arange(PB * K) < kept, terms[chosen], -1)
    shuffle = jax.random.permutation(streams[3], PB * K)
    return ranked[shuffle].reshape(PB, K)


def draw_term_ids(key, part):
    pieces = jax.random.split(jax.random.fold_in(key, 17), N_BATCH + 2)
    hot_owner = jax.random.randint(pieces[0], (), 0, N_BATCH * N_VOCAB)
    boosts = jax.random.randint(pieces[1], (N_BATCH * N_VOCAB,), 0, 512)
    shards = jax.vmap(lambda shard_key: shard_terms(shard_key, hot_owner, boosts))(pieces[2:])
    return shards.reshape(N_BATCH * PB, K).astype(jnp.int32)


def touch_ends(drawn, stream_key, low, top_value):
    dims = drawn.shape
    index_at = [jax.random.randint(jax.random.fold_in(stream_key, axis), (), 0, dims[axis]) for axis in range(len(dims))]
    drawn = drawn.at[tuple(index_at)].set(low)
    longest = dims.index(max(dims))
    index_at[longest] = (index_at[longest] + 1) % dims[longest]
    return drawn.at[tuple(index_at)].set(top_value)


def steps_of(stream_key, dims, cuts, smallest, high):
    def one(dim, parts):
        draws = jax.random.uniform(jax.random.fold_in(jax.random.fold_in(stream_key, 6), dim), (parts,), jnp.float32, smallest / len(cuts), high / len(cuts))
        return jnp.repeat(jnp.exp(draws), dims[dim] // parts).reshape((-1,) + (1,) * (len(dims) - dim - 1))

    factor_of = one(*cuts[0])
    for cut in cuts[1:]:
        factor_of = factor_of * one(*cut)
    return factor_of


def bell_draw(own_key, dims, scale, reach, cuts=(), held_as=jnp.bfloat16):
    values = scale * jax.random.normal(own_key, dims, jnp.float32)
    if cuts:
        values = values * steps_of(own_key, dims, cuts, -0.22, 0.18)
    return jnp.clip(values, -reach, reach).astype(held_as)


def setup_inputs(seed: int = 0) -> dict:
    splits = jax.random.split(jax.random.key(seed), 10)
    return {
        "hidden": draw_hidden(jax.random.fold_in(splits[9], 71), 0),
        "dense_w": bell_draw(splits[1], (MODEL_WIDTH, MODEL_WIDTH), MODEL_WIDTH ** -0.5, 0.21875),
        "dense_b": bell_draw(splits[2], (MODEL_WIDTH,), 0.5, 3.0, (), jnp.float32),
        "norm_gain": jnp.clip(1.0 + 0.1 * jax.random.normal(splits[3], (MODEL_WIDTH,), jnp.float32), 0.5, 1.5),
        "norm_bias": bell_draw(splits[4], (MODEL_WIDTH,), 0.3, 2.0, (), jnp.float32),
        "vocabulary_weight": bell_draw(splits[5], (MODEL_WIDTH, VOCAB_PADDED), MODEL_WIDTH ** -0.5, 0.21875, ((1, 16),)),
        "vocabulary_bias": bell_draw(splits[6], (VOCAB_PADDED,), 1.0, 5.0, ((0, 16),)),
        "lengths": touch_ends(jax.random.randint(splits[7], (PAS,), L // 8, L + 1), jax.random.fold_in(splits[7], 1), L // 8, L).astype(jnp.int32),
        "term_ids": draw_term_ids(jax.random.fold_in(splits[9], 71), 0),
    }


def transform_rows(token_rows, dense_w, dense_b, norm_gain, norm_bias):
    pre = jnp.dot(token_rows, dense_w, preferred_element_type=jnp.float32) + dense_b
    activated = jax.nn.gelu(pre, approximate=False)
    centered = activated - lax.optimization_barrier(jnp.mean(activated, axis=-1, keepdims=True))
    spread = lax.optimization_barrier(jnp.mean(centered * centered, axis=-1, keepdims=True))
    normed = centered * lax.rsqrt(spread + 1e-06) * norm_gain + norm_bias
    return normed.astype(jnp.bfloat16)

def reference(hidden, dense_w, dense_b, norm_gain, norm_bias, vocabulary_weight, vocabulary_bias, lengths, term_ids):
    passage_rows = hidden.reshape(PAS, L, MODEL_WIDTH)
    positions = jnp.arange(L).astype(jnp.int32)
    bias_wide = vocabulary_bias.astype(jnp.float32)

    def one_passage(passage_pair):
        token_rows, length = passage_pair
        normed = transform_rows(token_rows, dense_w, dense_b, norm_gain, norm_bias)
        logits = jnp.dot(normed, vocabulary_weight, preferred_element_type=jnp.float32) + bias_wide
        active = jnp.log1p(jnp.maximum(logits, 0.0))
        counted = (positions < length)[:, None]
        return lax.optimization_barrier(jnp.max(jnp.where(counted, active, 0.0), axis=0))
    vectors = lax.map(one_passage, (passage_rows, lengths))
    column_span = jnp.arange(VOCAB_PADDED).astype(jnp.int32)
    vectors = jnp.where(column_span[None, :] < VOCAB, vectors, 0.0)
    device_list = N_BATCH * N_VOCAB
    owner_width = VOCAB_PADDED // N_VOCAB
    flattened_terms = term_ids.reshape(-1)
    present = flattened_terms >= 0
    clamped_terms = jnp.where(present, flattened_terms, 0).astype(jnp.int32)
    passage_position = (jnp.arange(PAS * K) // K).astype(jnp.int32)
    picked = vectors[passage_position, clamped_terms]
    owners = (clamped_terms % device_list).astype(jnp.int32)
    sender_ids = (passage_position // PB * N_VOCAB + clamped_terms // owner_width).astype(jnp.int32)
    groups = sender_ids * device_list + owners

    def count_step(totals, group_pair):
        group_id, alive_flag = group_pair
        placed = totals[group_id]
        return (totals.at[group_id].add(alive_flag.astype(jnp.int32)), placed)
    finals, posting_slots = lax.scan(count_step, jnp.zeros((device_list * device_list,), jnp.int32), (groups, present))
    receiver_ids = jnp.where(present, owners, device_list).astype(jnp.int32)
    posting_weights = jnp.zeros((device_list, POSTING_LIMIT, device_list), jnp.float32).at[receiver_ids, posting_slots, sender_ids].set(picked, mode='drop')
    posting_key_codes = jnp.full((device_list, POSTING_LIMIT, device_list), -1, jnp.int32).at[receiver_ids, posting_slots, sender_ids].set((passage_position * VOCAB_PADDED + clamped_terms).astype(jnp.int32), mode='drop')
    return (vectors, posting_weights, posting_key_codes)
```

```python
import functools

import jax
import jax.numpy as jnp
from jax import lax
from jax.experimental import pallas as pl
from jax.experimental.pallas import tpu as pltpu
from jax.sharding import PartitionSpec as P

VOCAB = 30522
VOCAB_PADDED = 30720
L = 256
K = 128
LIMIT = 5
LANES = 128
BIG = 1 << 20


def transform_kernel(lengths_ref, hidden_ref, w_ref, b_ref, gain_ref, bias_ref, out_ref):
    pre = jnp.dot(hidden_ref[...], w_ref[...], preferred_element_type=jnp.float32) + b_ref[...]
    act = 0.5 * pre * (1.0 + lax.erf(pre * (0.5 ** 0.5)))
    centered = act - jnp.mean(act, axis=-1, keepdims=True)
    spread = jnp.mean(centered * centered, axis=-1, keepdims=True)
    normed = centered * lax.rsqrt(spread + 1e-06) * gain_ref[...] + bias_ref[...]
    places = lax.broadcasted_iota(jnp.int32, normed.shape, 0)
    limit = lengths_ref[pl.program_id(0)]
    normed = jnp.where(places < limit, normed, normed[0:1, :])
    out_ref[...] = normed.astype(jnp.bfloat16)


def transform(hidden, lengths2, dense_w, dense_b, norm_gain, norm_bias):
    rows, width = hidden.shape
    vec = pl.BlockSpec((1, width), lambda i, *_: (0, 0))
    return pl.pallas_call(
        transform_kernel,
        grid_spec=pltpu.PrefetchScalarGridSpec(
            num_scalar_prefetch=1,
            grid=(rows // L,),
            in_specs=[
                pl.BlockSpec((L, width), lambda i, *_: (i, 0)),
                pl.BlockSpec((width, width), lambda i, *_: (0, 0)),
                vec, vec, vec,
            ],
            out_specs=pl.BlockSpec((L, width), lambda i, *_: (i, 0)),
        ),
        out_shape=jax.ShapeDtypeStruct((rows, width), jnp.bfloat16),
    )(lengths2, hidden, dense_w, dense_b[None], norm_gain[None], norm_bias[None])


def pool_kernel(s_ref, w_ref, bias_ref, first_ref, out_ref, tops):
    passages = s_ref.shape[0] // L
    width = w_ref.shape[1]
    step = 640

    def body(n, _):
        c = pl.multiple_of(n * step, LANES)
        for r in range(passages):
            d = jnp.dot(s_ref[r * L:(r + 1) * L, :], w_ref[:, pl.ds(c, step)], preferred_element_type=jnp.float32)
            tops[r, :, pl.ds(c, step)] = jnp.max(d.reshape(L // 8, 8, step), axis=0)
        return 0

    lax.fori_loop(0, width // step, body, 0)
    best = jnp.max(tops[...], axis=1) + bias_ref[...].astype(jnp.float32)
    columns = first_ref[0] + lax.broadcasted_iota(jnp.int32, best.shape, 1)
    out_ref[...] = jnp.where(columns < VOCAB, jnp.log1p(jnp.maximum(best, 0.0)), 0.0)


def pool(gathered, columns_w, columns_b, first):
    rows, features = gathered.shape
    width = columns_w.shape[1]
    passages = rows // L
    per = 8
    return pl.pallas_call(
        pool_kernel,
        grid=(passages // per,),
        in_specs=[
            pl.BlockSpec((per * L, features), lambda i: (i, 0)),
            pl.BlockSpec((features, width), lambda i: (0, 0)),
            pl.BlockSpec((1, width), lambda i: (0, 0)),
            pl.BlockSpec(memory_space=pltpu.SMEM),
        ],
        out_specs=pl.BlockSpec((per, width), lambda i: (i, 0)),
        scratch_shapes=[pltpu.VMEM((per, 8, width), jnp.float32)],
        out_shape=jax.ShapeDtypeStruct((passages, width), jnp.float32),
        compiler_params=pltpu.CompilerParams(vmem_limit_bytes=48 * 2**20),
    )(gathered, columns_w, columns_b[None], first)


def pick_kernel(where_ref, terms_ref, vectors_ref, out_ref, codes):
    passages, places = terms_ref.shape
    first, first_passage = where_ref[0], where_ref[1]
    groups = vectors_ref.shape[1] // LANES
    out_ref[...] = jnp.zeros_like(out_ref)
    k_row = (lax.broadcasted_iota(jnp.int32, (1, places), 1) + 1).astype(jnp.float32)
    j_col = lax.broadcasted_iota(jnp.int32, (16, places), 0)
    o_col = lax.broadcasted_iota(jnp.int32, (LANES, places), 0)
    for p in range(passages):
        t = terms_ref[p:p + 1, :]
        rel = t - first
        j = jnp.where((t >= 0) & (rel >= 0), rel // LANES, 99)
        a = jnp.where(j_col == j, k_row, 0.0).astype(jnp.bfloat16)
        b = jnp.where(o_col == t % LANES, 1.0, 0.0).astype(jnp.bfloat16)
        found = lax.dot_general(a, b, (((1,), (1,)), ((), ())), preferred_element_type=jnp.float32)
        found = found.astype(jnp.int32)
        codes[:, p, :] = jnp.where(found > 0, p * places + found - 1, BIG)
    last = jnp.full((1, LANES), -1, jnp.int32)
    lane = lax.broadcasted_iota(jnp.int32, (passages, LANES), 1)
    row = lax.broadcasted_iota(jnp.int32, (passages, LANES), 0)
    for c in range(LIMIT):
        low = jnp.full((passages, LANES), BIG, jnp.int32)
        for j in range(groups):
            code = codes[j]
            low = jnp.minimum(low, jnp.where(code > last, code, BIG))
        low = jnp.min(low, axis=0, keepdims=True)
        weight = jnp.zeros((passages, LANES), jnp.float32)
        key = jnp.zeros((passages, LANES), jnp.int32)
        for j in range(groups):
            hit = (codes[j] == low) & (low < BIG)
            weight = weight + jnp.where(hit, vectors_ref[:, j * LANES:(j + 1) * LANES], 0.0)
            key = key + jnp.where(hit, (first_passage + row) * VOCAB_PADDED + first + j * LANES + lane + 1, 0)
        out_ref[c:c + 1, :] = jnp.sum(weight, axis=0, keepdims=True)
        out_ref[8 + c:9 + c, :] = (jnp.sum(key, axis=0, keepdims=True) - 1).astype(jnp.float32)
        last = low


def pick(term_ids, vectors, first, first_passage):
    where = jnp.stack([first, first_passage]).astype(jnp.int32)
    return pl.pallas_call(
        pick_kernel,
        in_specs=[pl.BlockSpec(memory_space=pltpu.SMEM)] + [pl.BlockSpec(memory_space=pltpu.VMEM)] * 2,
        out_specs=pl.BlockSpec(memory_space=pltpu.VMEM),
        scratch_shapes=[pltpu.VMEM((16,) + term_ids.shape, jnp.int32)],
        out_shape=jax.ShapeDtypeStruct((16, LANES), jnp.float32),
    )(where, term_ids, vectors)


def local(hidden, dense_w, dense_b, norm_gain, norm_bias, vocabulary_weight, vocabulary_bias, lengths, term_ids):
    passages = lengths.shape[0]
    width = vocabulary_weight.shape[1]
    v = lax.axis_index("vocab")
    b = lax.axis_index("batch")
    own = hidden.shape[0] // L
    mine = lax.dynamic_slice(lengths, (v * own,), (own,))
    states = transform(hidden, mine, dense_w, dense_b, norm_gain, norm_bias)
    gathered = lax.all_gather(states, "vocab", axis=0, tiled=True)
    first = v * width
    vectors = pool(gathered, vocabulary_weight, vocabulary_bias, first[None].astype(jnp.int32))
    sent = pick(term_ids, vectors, first, b * passages)
    got = lax.all_to_all(sent, ("batch", "vocab"), split_axis=1, concat_axis=1, tiled=True)
    return vectors, got[None, :LIMIT], got[None, 8:8 + LIMIT].astype(jnp.int32)


def solution(mesh):
    in_specs = (
        P(("batch", "vocab"), None), P(), P(), P(), P(),
        P(None, "vocab"), P("vocab"), P("batch"), P("batch", None),
    )
    out_specs = (P("batch", "vocab"), P(("batch", "vocab"), None, None), P(("batch", "vocab"), None, None))
    return jax.shard_map(local, mesh=mesh, in_specs=in_specs, out_specs=out_specs, check_vma=False)
```

```python
import jax
import jax.numpy as jnp
from jax import lax
from jax.experimental import pallas as pl
from jax.experimental.pallas import tpu as pltpu
from jax.sharding import PartitionSpec as P

VOCAB = 30522
VOCAB_PADDED = 30720
L = 256
K = 128
LIMIT = 5
LANES = 128
BIG = 1 << 20


MESH = pl.DeviceIdType.MESH
WIDE = 1024
PIECE = 512
DIRECT = 320
SLICE = 112
DELTA = (0, -1, 1, 2)
ORDER = (
    (0, 0),
    (1, 0), (0, 1), (1, 1),
    (2, 0), (2, 1), (0, 2), (1, 2), (2, 2),
    (3, 0), (3, 1), (3, 2), (0, 3), (1, 3), (2, 3), (3, 3),
)


def encode_kernel(
    lengths_ref, hidden_ref, dense_ref, b_ref, gain_ref, bias_ref, weight_ref, vbias_ref, out_ref,
    hid, den, states, weights, tops, pooled, landed, local_sem, send_sem, recv_sem,
):
    b, v = lax.axis_index("batch"), lax.axis_index("vocab")
    y, c = b // 2, b % 2
    x, z = v // 4, v % 4
    sign = 1 - 2 * c

    def device(dx=0, dy=0, dz=0, flip=0):
        core = 1 - c if flip else c
        return (2 * ((y + dy + 4) % 4) + core, 4 * ((x + dx + 4) % 4) + (z + dz + 4) % 4)

    def send(index, source, target, to):
        copy = pltpu.make_async_remote_copy(
            src_ref=source, dst_ref=target, send_sem=send_sem.at[index], recv_sem=recv_sem.at[index],
            device_id=to, device_id_type=MESH,
        )
        copy.start()

    def got(index, region):
        pltpu.make_async_remote_copy(
            src_ref=region, dst_ref=region, send_sem=send_sem.at[index], recv_sem=recv_sem.at[index],
            device_id=device(flip=1), device_id_type=MESH,
        ).wait_recv()

    def left(index, region):
        pltpu.make_async_remote_copy(
            src_ref=region, dst_ref=region, send_sem=send_sem.at[index], recv_sem=recv_sem.at[index],
            device_id=device(flip=1), device_id_type=MESH,
        ).wait_send()

    def y_rows(k):
        return pl.ds(pl.multiple_of(DIRECT + SLICE * ((y + k + 4) % 4), 16), SLICE)

    def kind_rows(kind):
        return y_rows(0) if kind == 0 else pl.ds(0, DIRECT)

    def w_at(r, j, rows):
        if r == 3:
            return weights.at[3, rows, pl.ds(PIECE * j, PIECE)]
        return weights.at[1 + j, rows, pl.ds(PIECE * (r - 1), PIECE)]

    def s_at(r, q):
        if r == 0:
            return states.at[0, 0, pl.ds(128 * q, 128)]
        return states.at[1 + q // 2, 0, pl.ds(256 * (r - 1) + 128 * (q % 2), 128)]

    def x_own(kind, j, side):
        return kind * 4 + j * 2 + side

    def x_fwd(kind, j):
        return 8 + kind * 2 + j

    def y_own(r, j, side):
        return 12 + (r - 1) * 4 + j * 2 + side

    def y_fwd(r, j):
        return 24 + (r - 1) * 2 + j

    def z_own(q, side):
        return 30 + q * 2 + side

    def z_fwd(h):
        return 38 + h

    def pair(s):
        return 40 + s

    def swap(r, flip):
        return 44 + r * 2 + flip

    wide_first = pl.multiple_of(c * (1920 - WIDE), LANES)
    load_h = pltpu.make_async_copy(hidden_ref, hid, local_sem.at[0])
    load_d = pltpu.make_async_copy(dense_ref, den, local_sem.at[1])
    load_w = pltpu.make_async_copy(weight_ref.at[:, pl.ds(wide_first, WIDE)], weights.at[0], local_sem.at[2])
    load_d.start()
    load_h.start()
    load_w.start()
    barrier = pltpu.get_barrier_semaphore()
    friends = [(dx, 0, 0, f) for dx in range(4) for f in range(2) if (dx, f) != (0, 0)]
    friends += [(0, 1, 0, 0), (0, -1, 0, 0), (0, 0, 1, 0), (0, 0, -1, 0)]
    for dx, dy, dz, f in friends:
        pl.semaphore_signal(barrier, inc=1, device_id=device(dx, dy, dz, f), device_id_type=MESH)
    pl.semaphore_wait(barrier, len(friends))

    def send_own_w(kind, j):
        for side, dx in ((0, 1), (1, -1)):
            send(
                x_own(kind, j, side),
                weight_ref.at[kind_rows(kind), pl.ds(pl.multiple_of(wide_first + PIECE * j, LANES), PIECE)],
                w_at(1 + side, j, kind_rows(kind)),
                device(dx=dx),
            )

    def fwd_w(kind, j):
        source = weights.at[1 + j, kind_rows(kind), pl.ds(pl.multiple_of(PIECE * c, LANES), PIECE)]
        send(x_fwd(kind, j), source, w_at(3, j, kind_rows(kind)), device(dx=sign))

    def got_own_w(kind, j):
        for side in range(2):
            got(x_own(kind, j, side), w_at(1 + side, j, kind_rows(kind)))

    def share_w(r, j):
        for side, dy in ((0, 1), (1, -1)):
            send(y_own(r, j, side), w_at(r, j, y_rows(0)), w_at(r, j, y_rows(0)), device(dy=dy))

    def relay_w(r, j):
        got(y_own(r, j, 0), w_at(r, j, y_rows(-1)))
        got(y_own(r, j, 1), w_at(r, j, y_rows(1)))
        send(y_fwd(r, j), w_at(r, j, y_rows(-sign)), w_at(r, j, y_rows(-sign)), device(dy=sign))

    def relayed_w(r, j):
        got(y_fwd(r, j), w_at(r, j, y_rows(2)))

    def send_own_s(q):
        for side, dz in ((0, 1), (1, -1)):
            send(z_own(q, side), s_at(0, q), s_at(1 + side, q), device(dz=dz))

    def relay_s(h):
        for q in (2 * h, 2 * h + 1):
            for side in range(2):
                got(z_own(q, side), s_at(1 + side, q))
        source = states.at[1 + h, 0, pl.ds(pl.multiple_of(256 * c, 256), 256)]
        send(z_fwd(h), source, states.at[3, 0, pl.ds(256 * h, 256)], device(dz=sign))

    def pair_s(s):
        send(pair(s), states.at[s, 0], states.at[s, 1], device(flip=1))

    def paired_s(s):
        got(pair(s), states.at[s, 1])

    send_own_w(0, 0)
    send_own_w(0, 1)
    send_own_w(1, 0)

    load_d.wait()
    load_h.wait()
    gain, shift, offset = gain_ref[...].reshape(1, -1), bias_ref[...].reshape(1, -1), b_ref[...].reshape(1, -1)

    def head(q, first):
        pre = jnp.dot(hid[128 * q:128 * q + 128, :], den[...], preferred_element_type=jnp.float32) + offset
        act = 0.5 * pre * (1.0 + lax.erf(pre * (0.5 ** 0.5)))
        centered = act - jnp.mean(act, axis=-1, keepdims=True)
        spread = jnp.mean(centered * centered, axis=-1, keepdims=True)
        normed = centered * lax.rsqrt(spread + 1e-06) * gain + shift
        if q % 2 == 0:
            first = normed[0:1, :]
        places = 128 * (q % 2) + lax.broadcasted_iota(jnp.int32, normed.shape, 0)
        normed = jnp.where(places < lengths_ref[2 * v + q // 2], normed, first)
        states[0, 0, 128 * q:128 * q + 128, :] = normed.astype(jnp.bfloat16)
        return first

    first = head(0, None)
    for q in range(1, 4):
        first = head(q, first)
        send_own_s(q - 1)
    load_w.wait()

    def event_0():
        got_own_w(0, 0)
        share_w(1, 0)
        share_w(2, 0)
        fwd_w(0, 0)
        send_own_s(3)
        pair_s(0)
        paired_s(0)

    def event_1():
        got_own_w(0, 1)
        share_w(1, 1)
        share_w(2, 1)
        fwd_w(0, 1)
        send_own_w(1, 1)
        relay_w(1, 0)
        relay_w(2, 0)
        relay_s(0)
        pair_s(1)
        paired_s(1)

    def event_2():
        got_own_w(1, 0)
        fwd_w(1, 0)
        relayed_w(1, 0)
        relayed_w(2, 0)

    def event_3():
        relay_w(1, 1)
        relay_w(2, 1)
        for j in range(2):
            got(x_fwd(0, j), w_at(3, j, kind_rows(0)))
            share_w(3, j)

    def event_4():
        relay_s(1)
        pair_s(2)
        paired_s(2)

    def event_6():
        relayed_w(1, 1)
        relayed_w(2, 1)
        got_own_w(1, 1)
        fwd_w(1, 1)

    def event_7():
        relay_w(3, 0)
        relay_w(3, 1)

    def event_9():
        for h in range(2):
            got(z_fwd(h), states.at[3, 0, pl.ds(256 * h, 256)])
        pair_s(3)
        paired_s(3)

    def event_12():
        for j in range(2):
            got(x_fwd(1, j), w_at(3, j, kind_rows(1)))
            relayed_w(3, j)

    events = {0: event_0, 1: event_1, 2: event_2, 3: event_3, 4: event_4, 6: event_6, 7: event_7, 9: event_9, 12: event_12}

    def step(n, _):
        for k, event in events.items():
            pl.when(n == k)(event)
        s = sum(jnp.where(n == k, sk, 0) for k, (sk, _) in enumerate(ORDER) if sk)
        w = sum(jnp.where(n == k, wk, 0) for k, (_, wk) in enumerate(ORDER) if wk)
        for cc in range(2):
            for piece in range(2):
                for hh in range(2):
                    d = jnp.dot(
                        states[s, cc, 256 * hh:256 * hh + 256, :],
                        weights[w, :, PIECE * piece:PIECE * piece + PIECE],
                        preferred_element_type=jnp.float32,
                    )
                    tops[w, s, cc, hh, :, PIECE * piece:PIECE * piece + PIECE] = jnp.max(d.reshape(32, 8, PIECE), axis=0)
        return 0

    lax.fori_loop(0, len(ORDER), step, 0)

    for s in range(4):
        for hh in range(2):
            r, h = ((0, hh), (1 + hh, 0), (1 + hh, 1), (3, hh))[s]
            row = 2 * ((z + DELTA[r] + 4) % 4) + h
            for cc in range(2):
                for w in range(4):
                    best = jnp.max(tops[w, s, cc, hh], axis=0, keepdims=True)
                    for piece in range(2):
                        slot, col = ((0, piece), (1 + piece, 0), (1 + piece, 1), (3, piece))[w]
                        pooled[slot, cc, pl.ds(row, 1), PIECE * col:PIECE * col + PIECE] = best[:, PIECE * piece:PIECE * piece + PIECE]
    back = (0, 2, 1, 3)
    for slot in (3, 1, 2, 0):
        for cc in range(2):
            if (slot, cc) != (0, 0):
                send(swap(slot, cc), pooled.at[slot, cc], landed.at[cc, back[slot]], device(dx=DELTA[slot], flip=cc))
    landed[0, 0] = pooled[0, 0]
    for slot in range(4):
        for cc in range(2):
            if (slot, cc) != (0, 0):
                got(swap(slot, cc), landed.at[cc, back[slot]])
    bias = vbias_ref[...].astype(jnp.float32)
    columns = 1920 * v + lax.broadcasted_iota(jnp.int32, (8, 1920), 1)
    for slot in range(4):
        raw = jnp.concatenate([landed[c, slot], landed[1 - c, slot][:, 2 * WIDE - 1920:]], axis=1) + bias
        done = jnp.where(columns < VOCAB, jnp.log1p(jnp.maximum(raw, 0.0)), 0.0)
        out_ref[pl.ds(pl.multiple_of(8 * ((x + DELTA[slot] + 4) % 4), 8), 8), :] = done

    for kind in range(2):
        for j in range(2):
            for side in range(2):
                left(x_own(kind, j, side), w_at(1 + side, j, kind_rows(kind)))
            left(x_fwd(kind, j), w_at(3, j, kind_rows(kind)))
    for r in range(1, 4):
        for j in range(2):
            for side in range(2):
                left(y_own(r, j, side), w_at(r, j, y_rows(0)))
            left(y_fwd(r, j), w_at(r, j, y_rows(0)))
    for q in range(4):
        for side in range(2):
            left(z_own(q, side), s_at(0, q))
    for h in range(2):
        left(z_fwd(h), states.at[3, 0, pl.ds(256 * h, 256)])
    for s in range(4):
        left(pair(s), states.at[s, 0])
    for slot in range(4):
        for cc in range(2):
            if (slot, cc) != (0, 0):
                left(swap(slot, cc), pooled.at[slot, cc])


MESSAGES = 52


def encode(hidden, dense_w, dense_b, norm_gain, norm_bias, vocabulary_weight, vocabulary_bias, lengths):
    anywhere = pl.BlockSpec(memory_space=pl.ANY)
    vmem = pl.BlockSpec(memory_space=pltpu.VMEM)
    return pl.pallas_call(
        encode_kernel,
        in_specs=[pl.BlockSpec(memory_space=pltpu.SMEM), anywhere, anywhere, vmem, vmem, vmem, anywhere, vmem],
        out_specs=vmem,
        out_shape=jax.ShapeDtypeStruct((32, 1920), jnp.float32),
        scratch_shapes=[
            pltpu.VMEM((512, 768), jnp.bfloat16),
            pltpu.VMEM((768, 768), jnp.bfloat16),
            pltpu.VMEM((4, 2, 512, 768), jnp.bfloat16),
            pltpu.VMEM((4, 768, WIDE), jnp.bfloat16),
            pltpu.VMEM((4, 4, 2, 2, 8, WIDE), jnp.float32),
            pltpu.VMEM((4, 2, 8, WIDE), jnp.float32),
            pltpu.VMEM((2, 4, 8, WIDE), jnp.float32),
            pltpu.SemaphoreType.DMA((3,)),
            pltpu.SemaphoreType.DMA((MESSAGES,)),
            pltpu.SemaphoreType.DMA((MESSAGES,)),
        ],
        compiler_params=pltpu.CompilerParams(collective_id=0, has_side_effects=True, vmem_limit_bytes=56 * 2**20),
    )(lengths, hidden, dense_w, dense_b, norm_gain, norm_bias, vocabulary_weight, vocabulary_bias[None])


def pick_kernel(where_ref, terms_ref, vectors_ref, out_ref, codes):
    passages, places = terms_ref.shape
    first, first_passage = where_ref[0], where_ref[1]
    groups = vectors_ref.shape[1] // LANES
    out_ref[...] = jnp.zeros_like(out_ref)
    k_row = (lax.broadcasted_iota(jnp.int32, (1, places), 1) + 1).astype(jnp.float32)
    j_col = lax.broadcasted_iota(jnp.int32, (16, places), 0)
    o_col = lax.broadcasted_iota(jnp.int32, (LANES, places), 0)
    for p in range(passages):
        t = terms_ref[p:p + 1, :]
        rel = t - first
        j = jnp.where((t >= 0) & (rel >= 0), rel // LANES, 99)
        a = jnp.where(j_col == j, k_row, 0.0).astype(jnp.bfloat16)
        b = jnp.where(o_col == t % LANES, 1.0, 0.0).astype(jnp.bfloat16)
        found = lax.dot_general(a, b, (((1,), (1,)), ((), ())), preferred_element_type=jnp.float32)
        found = found.astype(jnp.int32)
        codes[:, p, :] = jnp.where(found > 0, p * places + found - 1, BIG)
    last = jnp.full((1, LANES), -1, jnp.int32)
    lane = lax.broadcasted_iota(jnp.int32, (passages, LANES), 1)
    row = lax.broadcasted_iota(jnp.int32, (passages, LANES), 0)
    for c in range(LIMIT):
        low = jnp.full((passages, LANES), BIG, jnp.int32)
        for j in range(groups):
            code = codes[j]
            low = jnp.minimum(low, jnp.where(code > last, code, BIG))
        low = jnp.min(low, axis=0, keepdims=True)
        weight = jnp.zeros((passages, LANES), jnp.float32)
        key = jnp.zeros((passages, LANES), jnp.int32)
        for j in range(groups):
            hit = (codes[j] == low) & (low < BIG)
            weight = weight + jnp.where(hit, vectors_ref[:, j * LANES:(j + 1) * LANES], 0.0)
            key = key + jnp.where(hit, (first_passage + row) * VOCAB_PADDED + first + j * LANES + lane + 1, 0)
        out_ref[c:c + 1, :] = jnp.sum(weight, axis=0, keepdims=True)
        out_ref[8 + c:9 + c, :] = (jnp.sum(key, axis=0, keepdims=True) - 1).astype(jnp.float32)
        last = low


def pick(term_ids, vectors, first, first_passage):
    where = jnp.stack([first, first_passage]).astype(jnp.int32)
    return pl.pallas_call(
        pick_kernel,
        in_specs=[pl.BlockSpec(memory_space=pltpu.SMEM)] + [pl.BlockSpec(memory_space=pltpu.VMEM)] * 2,
        out_specs=pl.BlockSpec(memory_space=pltpu.VMEM),
        scratch_shapes=[pltpu.VMEM((16,) + term_ids.shape, jnp.int32)],
        out_shape=jax.ShapeDtypeStruct((16, LANES), jnp.float32),
    )(where, term_ids, vectors)


def local(hidden, dense_w, dense_b, norm_gain, norm_bias, vocabulary_weight, vocabulary_bias, lengths, term_ids):
    passages = lengths.shape[0]
    width = vocabulary_weight.shape[1]
    v = lax.axis_index("vocab")
    b = lax.axis_index("batch")
    vectors = encode(hidden, dense_w, dense_b, norm_gain, norm_bias, vocabulary_weight, vocabulary_bias, lengths)
    sent = pick(term_ids, vectors, v * width, b * passages)
    got = lax.all_to_all(sent, ("batch", "vocab"), split_axis=1, concat_axis=1, tiled=True)
    return vectors, got[None, :LIMIT], got[None, 8:8 + LIMIT].astype(jnp.int32)


def solution(mesh):
    in_specs = (
        P(("batch", "vocab"), None), P(), P(), P(), P(),
        P(None, "vocab"), P("vocab"), P("batch"), P("batch", None),
    )
    out_specs = (P("batch", "vocab"), P(("batch", "vocab"), None, None), P(("batch", "vocab"), None, None))
    return jax.shard_map(local, mesh=mesh, in_specs=in_specs, out_specs=out_specs, check_vma=False)
```

```python
import jax
import jax.numpy as jnp
from jax import lax
from jax.experimental import pallas as pl
from jax.experimental.pallas import tpu as pltpu
from jax.sharding import PartitionSpec as P

VOCAB = 30522
VOCAB_PADDED = 30720
K = 128
LIMIT = 5
LANES = 128
BIG = 1 << 20
MESH = pl.DeviceIdType.MESH
BLOCK = 1920
WIDE = 1024
PIECE = 512
DIRECT = 320
SLICE = 112
DELTA = (0, -1, 1, 2)

STEPS = (
    ((0, 0), (0, 1), (1, 0), (1, 1)),
    ((2, 0), (2, 1), (0, 2), (1, 2)),
    ((2, 2), (3, 0), (3, 1), (3, 2)),
    ((0, 3), (1, 3), (2, 3), (3, 3)),
    ((4, 0), (4, 1), (4, 2), (4, 3)),
    ((0, 4), (1, 4), (2, 4), (3, 4)),
    ((4, 4), (5, 0), (5, 1), (5, 2)),
    ((5, 3), (5, 4), (0, 5), (1, 5)),
    ((2, 5), (3, 5), (4, 5), (5, 5)),
    ((6, 0), (6, 1), (6, 2), (6, 3)),
    ((6, 4), (6, 5), (0, 6), (1, 6)),
    ((2, 6), (3, 6), (4, 6), (5, 6)),
    ((6, 6), (7, 0), (7, 1), (7, 2)),
    ((7, 3), (7, 4), (7, 5), (7, 6)),
    ((0, 7), (1, 7), (2, 7), (3, 7)),
    ((4, 7), (5, 7), (6, 7), (7, 7)),
)


class Numbers:
    def __init__(self):
        self.known = {}

    def __call__(self, *name):
        return self.known.setdefault(name, len(self.known))


def encode_kernel(
    lengths_ref, hidden_ref, dense_ref, b_ref, gain_ref, bias_ref, weight_ref, vbias_ref, terms_ref,
    out_ref, out_w_ref, out_k_ref,
    hid, den, states, weights, tops, pooled, landed, codes, lows, sheet, boxes, batch_in, vocab_out, vocab_in, sheet_in,
    local_sem, send_sem, recv_sem,
):
    b, v = lax.axis_index("batch"), lax.axis_index("vocab")
    y, c = b // 2, b % 2
    x, z = v // 4, v % 4
    sign = 1 - 2 * c
    number = Numbers()
    started = []

    def device(dx=0, dy=0, dz=0, flip=0):
        core = 1 - c if flip else c
        return (2 * ((y + dy + 4) % 4) + core, 4 * ((x + dx + 4) % 4) + (z + dz + 4) % 4)

    def copy(name, source, target, to):
        i = number(*name)
        return pltpu.make_async_remote_copy(
            src_ref=source, dst_ref=target, send_sem=send_sem.at[i], recv_sem=recv_sem.at[i],
            device_id=to, device_id_type=MESH,
        )

    def send(name, source, target, to):
        copy(name, source, target, to).start()
        started.append(name)

    def got(name, region):
        copy(name, region, region, device(flip=1)).wait_recv()

    def y_rows(k):
        return pl.ds(pl.multiple_of(DIRECT + SLICE * ((y + k + 4) % 4), 16), SLICE)

    def kind_rows(kind):
        return y_rows(0) if kind == 0 else pl.ds(0, DIRECT)

    wide_first = pl.multiple_of(c * (BLOCK - WIDE), LANES)
    load_h = pltpu.make_async_copy(hidden_ref, hid, local_sem.at[0])
    load_d = pltpu.make_async_copy(dense_ref, den, local_sem.at[1])
    load_w = [
        pltpu.make_async_copy(weight_ref.at[:, pl.ds(pl.multiple_of(wide_first + PIECE * i, LANES), PIECE)], weights.at[i], local_sem.at[2 + i])
        for i in range(2)
    ]
    load_d.start()
    load_h.start()
    for load in load_w:
        load.start()
    barrier = pltpu.get_barrier_semaphore()
    friends = [((b + d) % 8, v) for d in range(1, 8)] + [(b, (v + d) % 16) for d in range(1, 16)]
    friends += [device(dx, 0, 0, 1) for dx in range(1, 4)]
    for friend in friends:
        pl.semaphore_signal(barrier, inc=1, device_id=friend, device_id_type=MESH)

    def send_own_w(kind, j):
        for side, dx in ((0, 1), (1, -1)):
            send(
                ("x", kind, j, side),
                weight_ref.at[kind_rows(kind), pl.ds(pl.multiple_of(wide_first + 256 * j, LANES), 256)],
                weights.at[2 + j, kind_rows(kind), pl.ds(256 * side, 256)],
                device(dx=dx),
            )

    def got_own_w(kind, j):
        for side in range(2):
            got(("x", kind, j, side), weights.at[2 + j, kind_rows(kind), pl.ds(256 * side, 256)])

    def fwd_w(kind, i):
        for j in (2 * i, 2 * i + 1):
            source = weights.at[2 + j, kind_rows(kind), pl.ds(pl.multiple_of(256 * c, LANES), 256)]
            send(("xf", kind, j), source, weights.at[6 + i, kind_rows(kind), pl.ds(256 * (j % 2), 256)], device(dx=sign))

    def got_fwd_w(kind, i):
        for j in (2 * i, 2 * i + 1):
            got(("xf", kind, j), weights.at[6 + i, kind_rows(kind), pl.ds(256 * (j % 2), 256)])

    def share_w(m):
        for side, dy in ((0, 1), (1, -1)):
            send(("y", m, side), weights.at[m, y_rows(0)], weights.at[m, y_rows(0)], device(dy=dy))

    def relay_w(m):
        got(("y", m, 0), weights.at[m, y_rows(-1)])
        got(("y", m, 1), weights.at[m, y_rows(1)])
        send(("yf", m), weights.at[m, y_rows(-sign)], weights.at[m, y_rows(-sign)], device(dy=sign))

    def relayed_w(m):
        got(("yf", m), weights.at[m, y_rows(2)])

    def send_own_s(q):
        for side, dz in ((0, 1), (1, -1)):
            send(("z", q, side), states.at[0, pl.ds(128 * q, 128)], states.at[2 + q, pl.ds(128 * side, 128)], device(dz=dz))

    def got_own_s(q):
        for side in range(2):
            got(("z", q, side), states.at[2 + q, pl.ds(128 * side, 128)])

    def fwd_s(h):
        for q in (2 * h, 2 * h + 1):
            source = states.at[2 + q, pl.ds(pl.multiple_of(128 * c, 128), 128)]
            send(("zf", q), source, states.at[6 + h, pl.ds(128 * (q % 2), 128)], device(dz=sign))

    def got_fwd_s(h):
        for q in (2 * h, 2 * h + 1):
            got(("zf", q), states.at[6 + h, pl.ds(128 * (q % 2), 128)])

    def pair_s(k):
        if k == 1:
            send(("d", k), states.at[0], states.at[1], device(flip=1))
        else:
            send(("d", k), states.at[k, pl.ds(0, 256)], states.at[k, pl.ds(256, 256)], device(flip=1))

    def paired_s(k):
        got(("d", k), states.at[1] if k == 1 else states.at[k, pl.ds(256, 256)])

    gain, shift, offset = gain_ref[...].reshape(1, -1), bias_ref[...].reshape(1, -1), b_ref[...].reshape(1, -1)

    def head(q, first):
        pre = jnp.dot(hid[128 * q:128 * q + 128, :], den[...], preferred_element_type=jnp.float32) + offset
        act = 0.5 * pre * (1.0 + lax.erf(pre * (0.5 ** 0.5)))
        centered = act - jnp.mean(act, axis=-1, keepdims=True)
        spread = jnp.mean(centered * centered, axis=-1, keepdims=True)
        normed = centered * lax.rsqrt(spread + 1e-06) * gain + shift
        if q % 2 == 0:
            first = normed[0:1, :]
        places = 128 * (q % 2) + lax.broadcasted_iota(jnp.int32, normed.shape, 0)
        normed = jnp.where(places < lengths_ref[2 * v + q // 2], normed, first)
        states[0, 128 * q:128 * q + 128, :] = normed.astype(jnp.bfloat16)
        return first

    load_d.wait()
    load_h.wait()
    first = head(0, None)
    pl.semaphore_wait(barrier, len(friends))
    for kind, j in ((0, 0), (0, 1), (1, 0), (0, 2), (0, 3), (1, 1)):
        send_own_w(kind, j)
    for q in range(1, 4):
        first = head(q, first)
        send_own_s(q - 1)
    for load in load_w:
        load.wait()

    def find_codes():
        k_row = (lax.broadcasted_iota(jnp.int32, (1, K), 1) + 1).astype(jnp.float32)
        j_col = lax.broadcasted_iota(jnp.int32, (16, K), 0)
        o_col = lax.broadcasted_iota(jnp.int32, (LANES, K), 0)
        start = BLOCK * v
        for p in range(32):
            t = terms_ref[p:p + 1, :]
            rel = t - start
            group = jnp.where((t >= 0) & (rel >= 0), rel // LANES, 99)
            one = jnp.where(j_col == group, k_row, 0.0).astype(jnp.bfloat16)
            two = jnp.where(o_col == t % LANES, 1.0, 0.0).astype(jnp.bfloat16)
            found = lax.dot_general(one, two, (((1,), (1,)), ((), ())), preferred_element_type=jnp.float32).astype(jnp.int32)
            codes[:, p, :] = jnp.where(found > 0, p * K + found - 1, BIG)
        lane = lax.broadcasted_iota(jnp.int32, (32, LANES), 1)
        row = lax.broadcasted_iota(jnp.int32, (32, LANES), 0)
        sheet[...] = jnp.zeros_like(sheet)
        last = jnp.full((1, LANES), -1, jnp.int32)
        for slot in range(LIMIT):
            low = jnp.full((32, LANES), BIG, jnp.int32)
            for j in range(15):
                code = codes[j]
                low = jnp.minimum(low, jnp.where(code > last, code, BIG))
            low = jnp.min(low, axis=0, keepdims=True)
            key = jnp.zeros((32, LANES), jnp.int32)
            for j in range(15):
                hit = (codes[j] == low) & (low < BIG)
                key = key + jnp.where(hit, (32 * b + row) * VOCAB_PADDED + start + j * LANES + lane + 1, 0)
            sheet[8 + slot:9 + slot, :] = (jnp.sum(key, axis=0, keepdims=True) - 1).astype(jnp.float32)
            lows[slot:slot + 1, :] = low
            last = low

    back = (0, 2, 1, 3)

    def pool(slots):
        for r in range(4):
            for h in range(2):
                row = 2 * ((z + DELTA[r] + 4) % 4) + h
                for cc in range(2):
                    if r == 0:
                        parts = ((cc, 2 * h), (cc, 2 * h + 1))
                    elif r == 3:
                        parts = ((6 + h, 2 * cc), (6 + h, 2 * cc + 1))
                    else:
                        parts = ((2 + 2 * h, 2 * cc + r - 1), (3 + 2 * h, 2 * cc + r - 1))
                    for m in range(8):
                        slot = (0, 0, 1, 1, 1, 1, 3, 3)[m]
                        if slot not in slots:
                            continue
                        (k0, g0), (k1, g1) = parts
                        best = jnp.max(jnp.maximum(tops[m, k0, g0], tops[m, k1, g1]), axis=0, keepdims=True)
                        if slot == 1:
                            for i in range(2):
                                pooled[1 + i, cc, pl.ds(row, 1), 256 * (m - 2):256 * (m - 1)] = best[:, 256 * i:256 * i + 256]
                        else:
                            pooled[slot, cc, pl.ds(row, 1), PIECE * (m % 2):PIECE * (m % 2) + PIECE] = best

    def swap(slot):
        for cc in range(2):
            if (slot, cc) != (0, 0):
                send(("e", slot, cc), pooled.at[slot, cc], landed.at[cc, back[slot]], device(dx=DELTA[slot], flip=cc))

    def event_0():
        got_own_w(0, 0)
        share_w(2)
        got_own_w(0, 1)
        share_w(3)
        send_own_s(3)
        pair_s(1)
        fwd_w(0, 0)
        send_own_w(1, 2)
        paired_s(1)

    def event_1():
        got_own_s(0)
        pair_s(2)
        relay_w(2)
        got_own_w(0, 2)
        share_w(4)
        find_codes()
        relay_w(3)
        got_own_w(0, 3)
        share_w(5)
        fwd_w(0, 1)
        send_own_w(1, 3)
        got_own_s(1)
        pair_s(3)
        fwd_s(0)
        paired_s(2)
        got_own_w(1, 0)
        relayed_w(2)

    def event_2():
        paired_s(3)

    def event_3():
        got_own_w(1, 1)
        fwd_w(1, 0)
        relay_w(4)
        relayed_w(3)
        got_own_s(2)
        pair_s(4)

    def event_4():
        got_fwd_w(0, 0)
        share_w(6)
        paired_s(4)

    def event_5():
        relay_w(5)
        relayed_w(4)
        got_own_w(1, 2)

    def event_6():
        got_own_s(3)
        pair_s(5)
        fwd_s(1)
        got_fwd_w(0, 1)
        share_w(7)
        relay_w(6)
        paired_s(5)

    def event_7():
        relayed_w(5)
        got_own_w(1, 3)
        fwd_w(1, 1)

    def event_8():
        relay_w(7)
        got_fwd_s(0)
        pair_s(6)

    def event_9():
        paired_s(6)

    def event_10():
        relayed_w(6)
        got_fwd_w(1, 0)
        got_fwd_s(1)
        pair_s(7)

    def event_12():
        paired_s(7)

    def event_14():
        relayed_w(7)
        got_fwd_w(1, 1)
        pool((0, 1))
        swap(1)
        swap(2)
        swap(0)

    events = (
        event_0, event_1, event_2, event_3, event_4, event_5, event_6, event_7,
        event_8, event_9, event_10, None, event_12, None, event_14, None,
    )

    def step(n, _):
        for at, event in enumerate(events):
            if event is not None:
                pl.when(n == at)(event)
        for part in range(4):
            k = sum(jnp.where(n == at, items[part][0], 0) for at, items in enumerate(STEPS) if items[part][0])
            m = sum(jnp.where(n == at, items[part][1], 0) for at, items in enumerate(STEPS) if items[part][1])
            d = jnp.dot(states[k], weights[m], preferred_element_type=jnp.float32)
            tops[m, k] = jnp.max(d.reshape(4, 16, 8, PIECE), axis=1)
        return 0

    lax.fori_loop(0, len(STEPS), step, 0)
    pool((3,))
    swap(3)
    landed[0, 0] = pooled[0, 0]
    bias = vbias_ref[...].astype(jnp.float32)
    columns = BLOCK * v + lax.broadcasted_iota(jnp.int32, (8, BLOCK), 1)
    for slot in (0, 1, 2, 3):
        for cc in range(2):
            if (slot, cc) != (0, 0):
                got(("e", back[slot], cc), landed.at[cc, slot])
        raw = jnp.concatenate([landed[c, slot], landed[1 - c, slot][:, 2 * WIDE - BLOCK:]], axis=1) + bias
        done = jnp.where(columns < VOCAB, jnp.log1p(jnp.maximum(raw, 0.0)), 0.0)
        out_ref[pl.ds(pl.multiple_of(8 * ((x + DELTA[slot] + 4) % 4), 8), 8), :] = done

    for slot in range(LIMIT):
        low = lows[slot:slot + 1, :]
        weight = jnp.zeros((32, LANES), jnp.float32)
        for j in range(15):
            hit = (codes[j] == low) & (low < BIG)
            weight = weight + jnp.where(hit, out_ref[:, j * LANES:(j + 1) * LANES], 0.0)
        sheet[slot:slot + 1, :] = jnp.sum(weight, axis=0, keepdims=True)
    boxes[...] = jnp.transpose(sheet[...]).reshape(8, 16, LANES)
    for d in range(1, 8):
        to = (b + d) % 8
        send(("pb", d), boxes.at[to], batch_in.at[b], (to, v))
    batch_in[b] = boxes[b]
    for d in range(1, 8):
        got(("pb", d), batch_in.at[(b - d + 8) % 8])
    for origin in range(8):
        vocab_out[:, origin, :] = batch_in[origin]
    for d in range(1, 16):
        to = (v + d) % 16
        send(("pv", d), vocab_out.at[to], vocab_in.at[v], (b, to))
    vocab_in[v] = vocab_out[v]
    for d in range(1, 16):
        got(("pv", d), vocab_in.at[(v - d + 16) % 16])
    for origin in range(16):
        sheet_in[:, origin, :] = vocab_in[origin]
    result = jnp.transpose(sheet_in[...].reshape(LANES, LANES))
    out_w_ref[...] = result[0:LIMIT]
    out_k_ref[...] = result[8:8 + LIMIT].astype(jnp.int32)

    def shape_of(name):
        if name[0] in ("x", "xf"):
            return weights.at[2, pl.ds(0, DIRECT if name[1] else SLICE), pl.ds(0, 256)]
        return {
            "y": weights.at[2, pl.ds(0, SLICE)],
            "yf": weights.at[2, pl.ds(0, SLICE)],
            "z": states.at[0, pl.ds(0, 128)],
            "zf": states.at[0, pl.ds(0, 128)],
            "d": states.at[0] if name[1] == 1 else states.at[0, pl.ds(0, 256)],
            "e": pooled.at[0, 0],
            "pb": boxes.at[0],
            "pv": vocab_out.at[0],
        }[name[0]]

    for name in started:
        copy(name, shape_of(name), shape_of(name), device(flip=1)).wait_send()


MESSAGES = 96


def encode(hidden, dense_w, dense_b, norm_gain, norm_bias, vocabulary_weight, vocabulary_bias, lengths, term_ids):
    anywhere = pl.BlockSpec(memory_space=pl.ANY)
    vmem = pl.BlockSpec(memory_space=pltpu.VMEM)
    smem = pl.BlockSpec(memory_space=pltpu.SMEM)
    return pl.pallas_call(
        encode_kernel,
        in_specs=[smem, anywhere, anywhere, vmem, vmem, vmem, anywhere, vmem, vmem],
        out_specs=[vmem, vmem, vmem],
        out_shape=[
            jax.ShapeDtypeStruct((32, BLOCK), jnp.float32),
            jax.ShapeDtypeStruct((LIMIT, LANES), jnp.float32),
            jax.ShapeDtypeStruct((LIMIT, LANES), jnp.int32),
        ],
        scratch_shapes=[
            pltpu.VMEM((512, 768), jnp.bfloat16),
            pltpu.VMEM((768, 768), jnp.bfloat16),
            pltpu.VMEM((8, 512, 768), jnp.bfloat16),
            pltpu.VMEM((8, 768, PIECE), jnp.bfloat16),
            pltpu.VMEM((8, 8, 4, 8, PIECE), jnp.float32),
            pltpu.VMEM((4, 2, 8, WIDE), jnp.float32),
            pltpu.VMEM((2, 4, 8, WIDE), jnp.float32),
            pltpu.VMEM((16, 32, LANES), jnp.int32),
            pltpu.VMEM((8, LANES), jnp.int32),
            pltpu.VMEM((LANES, LANES), jnp.float32),
            pltpu.VMEM((8, 16, LANES), jnp.float32),
            pltpu.VMEM((8, 16, LANES), jnp.float32),
            pltpu.VMEM((16, 8, LANES), jnp.float32),
            pltpu.VMEM((16, 8, LANES), jnp.float32),
            pltpu.VMEM((8, 16, LANES), jnp.float32),
            pltpu.SemaphoreType.DMA((4,)),
            pltpu.SemaphoreType.DMA((MESSAGES,)),
            pltpu.SemaphoreType.DMA((MESSAGES,)),
        ],
        compiler_params=pltpu.CompilerParams(collective_id=0, has_side_effects=True, vmem_limit_bytes=56 * 2**20),
    )(lengths, hidden, dense_w, dense_b, norm_gain, norm_bias, vocabulary_weight, vocabulary_bias, term_ids)


def local(hidden, dense_w, dense_b, norm_gain, norm_bias, vocabulary_weight, vocabulary_bias, lengths, term_ids):
    vectors, weights, keys = encode(
        hidden, dense_w, dense_b, norm_gain, norm_bias, vocabulary_weight, vocabulary_bias[None], lengths, term_ids
    )
    return vectors, weights[None], keys[None]


def solution(mesh):
    in_specs = (
        P(("batch", "vocab"), None), P(), P(), P(), P(),
        P(None, "vocab"), P("vocab"), P("batch"), P("batch", None),
    )
    out_specs = (P("batch", "vocab"), P(("batch", "vocab"), None, None), P(("batch", "vocab"), None, None))
    return jax.shard_map(local, mesh=mesh, in_specs=in_specs, out_specs=out_specs, check_vma=False)
```

```python
import jax
import jax.numpy as jnp
from jax import lax
from jax.experimental import pallas as pl
from jax.experimental.pallas import tpu as pltpu
from jax.sharding import PartitionSpec as P

VOCAB = 30522
VOCAB_PADDED = 30720
K = 128
LIMIT = 5
LANES = 128
BIG = 1 << 20
MESH = pl.DeviceIdType.MESH
BLOCK = 1920
WIDE = 1024
PIECE = 512
DIRECT = (640, 256, 256, 256)
SLICE = tuple((768 - rows) // 4 for rows in DIRECT)
DELTA = (0, -1, 1, 2)

FIRST = (
    ((("own_s", 3), ("pair", 1)), ((0, 0), (0, 1))),
    ((("share", 2), ("share", 3), ("rows", 1)), ((1, 0), (1, 1))),
)
FOURS = (
    (
        (("across", 0, 0), ("own_w", 1, 2), ("codes",), ("relay", 2), ("pair", 2), ("rows", 2), ("relay", 3), ("columns", 2)),
        ((0, 2), (1, 2), (2, 0), (2, 1)),
    ),
    ((("share", 4), ("pair", 3), ("far", 0), ("rows", 3)), ((2, 2), (3, 0), (3, 1), (3, 2))),
    (
        (("share", 5), ("across", 0, 1), ("own_w", 1, 3), ("pair", 4), ("columns", 3)),
        ((0, 3), (1, 3), (2, 3), (3, 3)),
    ),
    ((("across", 1, 0), ("relay", 4), ("rows", 4)), ((4, 0), (4, 1), (4, 2), (4, 3))),
    ((("pair", 5), ("far", 1), ("relay", 5), ("share", 6), ("columns", 4)), ((0, 4), (1, 4), (2, 4), (3, 4))),
    ((("share", 7), ("across", 1, 1), ("rows", 5)), ((4, 4), (5, 0), (5, 1), (5, 2))),
)
EIGHTS = (
    (
        (("relay", 6), ("columns", 5), ("pair", 6)),
        ((5, 3), (5, 4), (0, 5), (1, 5), (2, 5), (3, 5), (4, 5), (5, 5)),
    ),
    (
        (("relay", 7), ("rows", 6), ("columns", 6), ("pair", 7)),
        ((6, 0), (6, 1), (6, 2), (6, 3), (6, 4), (6, 5), (0, 6), (1, 6)),
    ),
    ((("rows", 7),), ((2, 6), (3, 6), (4, 6), (5, 6), (6, 6), (7, 0), (7, 1), (7, 2))),
    ((("columns", 7),), ((7, 3), (7, 4), (7, 5), (7, 6), (0, 7), (1, 7), (2, 7), (3, 7))),
)
LAST = (((("early",),), ((4, 7), (5, 7), (6, 7), (7, 7))),)


class Numbers:
    def __init__(self):
        self.known = {}

    def __call__(self, *name):
        return self.known.setdefault(name, len(self.known))


def encode_kernel(
    lengths_ref, hidden_ref, dense_ref, b_ref, gain_ref, bias_ref, weight_ref, vbias_ref, terms_ref,
    out_ref, sheet_out_ref,
    hid, den, states, weights, tops, pooled, landed, codes, lows, sheet, boxes, batch_in, vocab_out, vec,
    local_sem, send_sem, recv_sem,
):
    b, v = lax.axis_index("batch"), lax.axis_index("vocab")
    y, c = b // 2, b % 2
    x, z = v // 4, v % 4
    sign = 1 - 2 * c
    number = Numbers()
    started = []

    def device(dx=0, dy=0, dz=0, flip=0):
        core = 1 - c if flip else c
        return (2 * ((y + dy + 4) % 4) + core, 4 * ((x + dx + 4) % 4) + (z + dz + 4) % 4)

    def copy(name, source, target, to):
        i = number(*name)
        assert i < MESSAGES
        return pltpu.make_async_remote_copy(
            src_ref=source, dst_ref=target, send_sem=send_sem.at[i], recv_sem=recv_sem.at[i],
            device_id=to, device_id_type=MESH,
        )

    def send(name, source, target, to):
        copy(name, source, target, to).start()
        if name not in started:
            started.append(name)

    waited = []

    def once(name, act):
        if name not in waited:
            waited.append(name)
            act()

    def got(name, region):
        copy(name, region, region, device(flip=1)).wait_recv()

    def y_rows(j, k):
        return pl.ds(pl.multiple_of(DIRECT[j] + SLICE[j] * ((y + k + 4) % 4), 16), SLICE[j])

    def kind_rows(kind, j):
        return y_rows(j, 0) if kind == 0 else pl.ds(0, DIRECT[j])

    def by_core(j, act):
        if j:
            act(0, 256)
        else:
            pl.when(c == 0)(lambda: act(0, 256))
            pl.when(c == 1)(lambda: act(128, 128))

    wide_first = pl.multiple_of(c * (BLOCK - WIDE), LANES)
    load_h = pltpu.make_async_copy(hidden_ref, hid, local_sem.at[0])
    load_d = pltpu.make_async_copy(dense_ref, den, local_sem.at[1])
    load_w = [
        pltpu.make_async_copy(weight_ref.at[:, pl.ds(pl.multiple_of(wide_first + PIECE * i, LANES), PIECE)], weights.at[i], local_sem.at[2 + i])
        for i in range(2)
    ]
    load_d.start()
    load_h.start()
    for load in load_w:
        load.start()
    barrier = pltpu.get_barrier_semaphore()
    friends = [((b + d) % 8, v) for d in range(1, 8)] + [(b, (v + d) % 16) for d in range(1, 16)]
    friends += [device(dx, 0, 0, 1) for dx in range(1, 4)]
    for friend in friends:
        pl.semaphore_signal(barrier, inc=1, device_id=friend, device_id_type=MESH)

    def send_own_w(kind, j):
        def act(first, width):
            for side, dx in ((0, 1), (1, -1)):
                send(
                    ("x", kind, j, side),
                    weights.at[j // 2, kind_rows(kind, j), pl.ds(256 * (j % 2) + first, width)],
                    weights.at[2 + j, kind_rows(kind, j), pl.ds(256 * side + first, width)],
                    device(dx=dx),
                )

        by_core(j, act)

    def got_own_w(kind, j):
        def act(first, width):
            for side in range(2):
                got(("x", kind, j, side), weights.at[2 + j, kind_rows(kind, j), pl.ds(256 * side + first, width)])

        once(("x", kind, j), lambda: by_core(j, act))

    def fwd_w(kind, i):
        for j in (2 * i, 2 * i + 1):
            got_own_w(kind, j)

            def act(first, width):
                source = weights.at[2 + j, kind_rows(kind, j), pl.ds(pl.multiple_of(256 * c + first, LANES), width)]
                target = weights.at[6 + i, kind_rows(kind, j), pl.ds(256 * (j % 2) + first, width)]
                send(("xf", kind, j), source, target, device(dx=sign))

            by_core(j, act)

    def got_fwd_w(kind, i):
        for j in (2 * i, 2 * i + 1):
            by_core(j, lambda first, width: got(("xf", kind, j), weights.at[6 + i, kind_rows(kind, j), pl.ds(256 * (j % 2) + first, width)]))

    def strips(m):
        return ((m - 2, 0), (m - 2, 256)) if m < 6 else ((2 * m - 12, 0), (2 * m - 11, 256))

    def share_w(m):
        got_own_w(0, m - 2) if m < 6 else got_fwd_w(0, m - 6)
        for j, at in strips(m):
            def act(first, width):
                piece = weights.at[m, y_rows(j, 0), pl.ds(at + first, width)]
                for side, dy in ((0, 1), (1, -1)):
                    send(("y", m, at, side), piece, piece, device(dy=dy))

            by_core(j, act)

    def relay_w(m):
        for j, at in strips(m):
            def act(first, width):
                got(("y", m, at, 0), weights.at[m, y_rows(j, -1), pl.ds(at + first, width)])
                got(("y", m, at, 1), weights.at[m, y_rows(j, 1), pl.ds(at + first, width)])
                piece = weights.at[m, y_rows(j, -sign), pl.ds(at + first, width)]
                send(("yf", m, at), piece, piece, device(dy=sign))

            by_core(j, act)

    def ready_w(m):
        for j, at in strips(m):
            by_core(j, lambda first, width: got(("yf", m, at), weights.at[m, y_rows(j, 2), pl.ds(at + first, width)]))
        got_own_w(1, m - 2) if m < 6 else got_fwd_w(1, m - 6)

    def send_own_s(q):
        for side, dz in ((0, 1), (1, -1)):
            send(("z", q, side), states.at[0, pl.ds(128 * q, 128)], states.at[2 + q, pl.ds(128 * side, 128)], device(dz=dz))

    def got_own_s(q):
        def act():
            for side in range(2):
                got(("z", q, side), states.at[2 + q, pl.ds(128 * side, 128)])

        once(("z", q), act)

    def fwd_s(h):
        for q in (2 * h, 2 * h + 1):
            got_own_s(q)
            source = states.at[2 + q, pl.ds(pl.multiple_of(128 * c, 128), 128)]
            send(("zf", q), source, states.at[6 + h, pl.ds(128 * (q % 2), 128)], device(dz=sign))

    def got_fwd_s(h):
        for q in (2 * h, 2 * h + 1):
            got(("zf", q), states.at[6 + h, pl.ds(128 * (q % 2), 128)])

    def pair_s(k):
        if k >= 6:
            got_fwd_s(k - 6)
        elif k >= 2:
            got_own_s(k - 2)
        if k == 1:
            send(("d", k), states.at[0], states.at[1], device(flip=1))
        else:
            send(("d", k), states.at[k, pl.ds(0, 256)], states.at[k, pl.ds(256, 256)], device(flip=1))

    def paired_s(k):
        got(("d", k), states.at[1] if k == 1 else states.at[k, pl.ds(256, 256)])

    gain, shift, offset = gain_ref[...].reshape(1, -1), bias_ref[...].reshape(1, -1), b_ref[...].reshape(1, -1)

    def head(q, first):
        pre = jnp.dot(hid[128 * q:128 * q + 128, :], den[...], preferred_element_type=jnp.float32) + offset
        act = 0.5 * pre * (1.0 + lax.erf(pre * (0.5 ** 0.5)))
        centered = act - jnp.mean(act, axis=-1, keepdims=True)
        spread = jnp.mean(centered * centered, axis=-1, keepdims=True)
        normed = centered * lax.rsqrt(spread + 1e-06) * gain + shift
        if q % 2 == 0:
            first = normed[0:1, :]
        places = 128 * (q % 2) + lax.broadcasted_iota(jnp.int32, normed.shape, 0)
        normed = jnp.where(places < lengths_ref[2 * v + q // 2], normed, first)
        states[0, 128 * q:128 * q + 128, :] = normed.astype(jnp.bfloat16)
        return first

    load_d.wait()
    load_h.wait()
    first = head(0, None)
    for load in load_w:
        load.wait()
    pl.semaphore_wait(barrier, len(friends))
    for kind, j in ((0, 0), (0, 1), (1, 0), (0, 2), (0, 3), (1, 1)):
        send_own_w(kind, j)
    send_own_s(0)
    for q in range(1, 4):
        first = head(q, first)
        if q > 1:
            send_own_s(q - 1)

    def find_codes():
        k_row = (lax.broadcasted_iota(jnp.int32, (1, K), 1) + 1).astype(jnp.float32)
        j_col = lax.broadcasted_iota(jnp.int32, (16, K), 0)
        o_col = lax.broadcasted_iota(jnp.int32, (LANES, K), 0)
        start = BLOCK * v
        for p in range(32):
            t = terms_ref[p:p + 1, :]
            rel = t - start
            group = jnp.where((t >= 0) & (rel >= 0), rel // LANES, 99)
            one = jnp.where(j_col == group, k_row, 0.0).astype(jnp.bfloat16)
            two = jnp.where(o_col == t % LANES, 1.0, 0.0).astype(jnp.bfloat16)
            found = lax.dot_general(one, two, (((1,), (1,)), ((), ())), preferred_element_type=jnp.float32).astype(jnp.int32)
            codes[:, p, :] = jnp.where(found > 0, p * K + found - 1, BIG)
        lane = lax.broadcasted_iota(jnp.int32, (32, LANES), 1)
        row = lax.broadcasted_iota(jnp.int32, (32, LANES), 0)
        sheet[...] = jnp.zeros_like(sheet)
        last = jnp.full((1, LANES), -1, jnp.int32)
        for slot in range(LIMIT):
            low = jnp.full((32, LANES), BIG, jnp.int32)
            for j in range(15):
                code = codes[j]
                low = jnp.minimum(low, jnp.where(code > last, code, BIG))
            low = jnp.min(low, axis=0, keepdims=True)
            key = jnp.zeros((32, LANES), jnp.int32)
            for j in range(15):
                hit = (codes[j] == low) & (low < BIG)
                key = key + jnp.where(hit, (32 * b + row) * VOCAB_PADDED + start + j * LANES + lane + 1, 0)
            sheet[8 + slot:9 + slot, :] = (jnp.sum(key, axis=0, keepdims=True) - 1).astype(jnp.float32)
            lows[slot:slot + 1, :] = low
            last = low

    back = (0, 2, 1, 3)

    def pool(slots):
        for r in range(4):
            for h in range(2):
                row = 2 * ((z + DELTA[r] + 4) % 4) + h
                for cc in range(2):
                    if r == 0:
                        parts = ((cc, 2 * h), (cc, 2 * h + 1))
                    elif r == 3:
                        parts = ((6 + h, 2 * cc), (6 + h, 2 * cc + 1))
                    else:
                        parts = ((2 + 2 * h, 2 * cc + r - 1), (3 + 2 * h, 2 * cc + r - 1))
                    for m in range(8):
                        slot = (0, 0, 1, 1, 1, 1, 3, 3)[m]
                        if slot not in slots:
                            continue
                        (k0, g0), (k1, g1) = parts
                        best = jnp.max(jnp.maximum(tops[m, k0, g0], tops[m, k1, g1]), axis=0, keepdims=True)
                        if slot == 1:
                            for i in range(2):
                                pooled[1 + i, cc, pl.ds(row, 1), 256 * (m - 2):256 * (m - 1)] = best[:, 256 * i:256 * i + 256]
                        else:
                            pooled[slot, cc, pl.ds(row, 1), PIECE * (m % 2):PIECE * (m % 2) + PIECE] = best

    def swap(slot):
        for cc in range(2):
            if (slot, cc) != (0, 0):
                send(("e", slot, cc), pooled.at[slot, cc], landed.at[cc, back[slot]], device(dx=DELTA[slot], flip=cc))

    def early():
        pool((0, 1))
        for slot in (1, 2, 0):
            swap(slot)

    acts = {
        "own_s": send_own_s, "own_w": send_own_w, "pair": pair_s, "rows": paired_s, "far": fwd_s,
        "share": share_w, "relay": relay_w, "columns": ready_w, "across": fwd_w, "codes": find_codes, "early": early,
    }

    def handle(todo):
        for name, *values in todo:
            acts[name](*values)

    def multiply(k, m):
        d = jnp.dot(states[k], weights[m], preferred_element_type=jnp.float32)
        tops[m, k] = jnp.max(d.reshape(4, 16, 8, PIECE), axis=1)

    def straight(table):
        for todo, pairs in table:
            handle(todo)
            for k, m in pairs:
                multiply(k, m)

    def looped(table):
        def step(n, _):
            for at, (todo, _) in enumerate(table):
                pl.when(n == at)(lambda: handle(todo))
            for part in range(len(table[0][1])):
                k, m = (
                    sum(jnp.where(n == at, pairs[part][i], 0) for at, (_, pairs) in enumerate(table) if pairs[part][i])
                    for i in range(2)
                )
                multiply(k, m)
            return 0

        lax.fori_loop(0, len(table), step, 0)

    straight(FIRST)
    looped(FOURS)
    looped(EIGHTS)
    straight(LAST)
    pool((3,))
    swap(3)
    landed[0, 0] = pooled[0, 0]

    def shape_of(name, width):
        if name[0] in ("x", "xf"):
            return weights.at[2, pl.ds(0, DIRECT[name[2]] if name[1] else SLICE[name[2]]), pl.ds(0, width)]
        if name[0] in ("y", "yf"):
            return weights.at[2, pl.ds(0, SLICE[dict((at, j) for j, at in strips(name[1]))[name[2]]]), pl.ds(0, width)]
        return {
            "z": states.at[0, pl.ds(0, 128)],
            "zf": states.at[0, pl.ds(0, 128)],
            "d": states.at[0] if name[1] == 1 else states.at[0, pl.ds(0, 256)],
            "e": pooled.at[0, 0],
            "pb": boxes.at[0],
            "pv": vocab_out.at[0],
        }[name[0]]

    def quarter_of(name):
        if name[0] in ("x", "xf"):
            return name[2]
        if name[0] in ("y", "yf"):
            return dict((at, j) for j, at in strips(name[1]))[name[2]]
        return 1

    def leave(name):
        by_core(quarter_of(name), lambda first, width: copy(name, shape_of(name, width), shape_of(name, width), device(flip=1)).wait_send())

    for name in [name for name in started if name[0] != "e"]:
        leave(name)
        started.remove(name)
    bias = vbias_ref[...].astype(jnp.float32).reshape(1, -1)
    columns = BLOCK * v + lax.broadcasted_iota(jnp.int32, (8, BLOCK), 1)
    for slot in (0, 1, 2, 3):
        for cc in range(2):
            if (slot, cc) != (0, 0):
                got(("e", back[slot], cc), landed.at[cc, slot])
        raw = jnp.concatenate([landed[c, slot], landed[1 - c, slot][:, 2 * WIDE - BLOCK:]], axis=1) + bias
        done = jnp.where(columns < VOCAB, jnp.log1p(jnp.maximum(raw, 0.0)), 0.0)
        vec[pl.ds(pl.multiple_of(8 * ((x + DELTA[slot] + 4) % 4), 8), 8), :] = done

    for slot in range(LIMIT):
        low = lows[slot:slot + 1, :]
        weight = jnp.zeros((32, LANES), jnp.float32)
        for j in range(15):
            hit = (codes[j] == low) & (low < BIG)
            weight = weight + jnp.where(hit, vec[:, j * LANES:(j + 1) * LANES], 0.0)
        sheet[slot:slot + 1, :] = jnp.sum(weight, axis=0, keepdims=True)
    store = pltpu.make_async_copy(vec, out_ref, local_sem.at[4])
    store.start()
    boxes[...] = jnp.transpose(sheet[...]).reshape(8, 16, LANES)
    for d in range(1, 8):
        to = (b + d) % 8
        send(("pb", d), boxes.at[to], batch_in.at[b], (to, v))
    batch_in[b] = boxes[b]
    for d in range(1, 8):
        got(("pb", d), batch_in.at[(b - d + 8) % 8])
    for origin in range(8):
        vocab_out[:, origin, :] = batch_in[origin]
    for d in range(1, 16):
        to = (v + d) % 16
        send(("pv", d), vocab_out.at[to], sheet_out_ref.at[v], (b, to))
    sheet_out_ref[v] = vocab_out[v]
    for d in range(1, 16):
        got(("pv", d), sheet_out_ref.at[(v - d + 16) % 16])

    store.wait()
    for name in started:
        leave(name)


MESSAGES = 112


def encode(hidden, dense_w, dense_b, norm_gain, norm_bias, vocabulary_weight, vocabulary_bias, lengths, term_ids):
    anywhere = pl.BlockSpec(memory_space=pl.ANY)
    vmem = pl.BlockSpec(memory_space=pltpu.VMEM)
    smem = pl.BlockSpec(memory_space=pltpu.SMEM)
    return pl.pallas_call(
        encode_kernel,
        in_specs=[smem, anywhere, anywhere, vmem, vmem, vmem, anywhere, vmem, vmem],
        out_specs=[anywhere, vmem],
        out_shape=[
            jax.ShapeDtypeStruct((32, BLOCK), jnp.float32),
            jax.ShapeDtypeStruct((16, 8, LANES), jnp.float32),
        ],
        scratch_shapes=[
            pltpu.VMEM((512, 768), jnp.bfloat16),
            pltpu.VMEM((768, 768), jnp.bfloat16),
            pltpu.VMEM((8, 512, 768), jnp.bfloat16),
            pltpu.VMEM((8, 768, PIECE), jnp.bfloat16),
            pltpu.VMEM((8, 8, 4, 8, PIECE), jnp.float32),
            pltpu.VMEM((4, 2, 8, WIDE), jnp.float32),
            pltpu.VMEM((2, 4, 8, WIDE), jnp.float32),
            pltpu.VMEM((16, 32, LANES), jnp.int32),
            pltpu.VMEM((8, LANES), jnp.int32),
            pltpu.VMEM((LANES, LANES), jnp.float32),
            pltpu.VMEM((8, 16, LANES), jnp.float32),
            pltpu.VMEM((8, 16, LANES), jnp.float32),
            pltpu.VMEM((16, 8, LANES), jnp.float32),
            pltpu.VMEM((32, BLOCK), jnp.float32),
            pltpu.SemaphoreType.DMA((5,)),
            pltpu.SemaphoreType.DMA((MESSAGES,)),
            pltpu.SemaphoreType.DMA((MESSAGES,)),
        ],
        compiler_params=pltpu.CompilerParams(collective_id=0, has_side_effects=True, vmem_limit_bytes=56 * 2**20),
    )(lengths, hidden, dense_w, dense_b, norm_gain, norm_bias, vocabulary_weight, vocabulary_bias, term_ids)


def finish_kernel(vectors_ref, sheet_ref, out_ref, out_w_ref, out_k_ref, rows):
    out_ref[...] = vectors_ref[...]
    for origin in range(16):
        rows[:, origin, :] = sheet_ref[origin]
    result = jnp.transpose(rows[...].reshape(LANES, LANES))
    out_w_ref[:, 0, :] = result[0:LIMIT]
    out_k_ref[:, 0, :] = result[8:8 + LIMIT].astype(jnp.int32)


def finish(vectors, sheet):
    vmem = pl.BlockSpec(memory_space=pltpu.VMEM)
    return pl.pallas_call(
        finish_kernel,
        in_specs=[vmem, vmem],
        out_specs=[vmem, vmem, vmem],
        out_shape=[
            jax.ShapeDtypeStruct(vectors.shape, jnp.float32),
            jax.ShapeDtypeStruct((LIMIT, 1, LANES), jnp.float32),
            jax.ShapeDtypeStruct((LIMIT, 1, LANES), jnp.int32),
        ],
        scratch_shapes=[pltpu.VMEM((8, 16, LANES), jnp.float32)],
    )(vectors, sheet)


def local(hidden, dense_w, dense_b, norm_gain, norm_bias, vocabulary_weight, vocabulary_bias, lengths, term_ids):
    vectors, sheet = encode(
        hidden, dense_w, dense_b, norm_gain, norm_bias, vocabulary_weight, vocabulary_bias, lengths, term_ids
    )
    vectors, weights, keys = finish(vectors, sheet)
    return vectors, jnp.swapaxes(weights, 0, 1), jnp.swapaxes(keys, 0, 1)


def solution(mesh):
    in_specs = (
        P(("batch", "vocab"), None), P(), P(), P(), P(),
        P(None, "vocab"), P("vocab"), P("batch"), P("batch", None),
    )
    out_specs = (P("batch", "vocab"), P(("batch", "vocab"), None, None), P(("batch", "vocab"), None, None))
    return jax.shard_map(local, mesh=mesh, in_specs=in_specs, out_specs=out_specs, check_vma=False)
```

```python
import jax
import jax.numpy as jnp
from jax import lax
from jax.experimental import pallas as pl
from jax.experimental.pallas import tpu as pltpu
from jax.sharding import PartitionSpec as P

VOCAB = 30522
VOCAB_PADDED = 30720
K = 128
LIMIT = 5
LANES = 128
BIG = 1 << 20
MESH = pl.DeviceIdType.MESH
BLOCK = 1920
WIDE = 1024
PIECE = 512
DIRECT = (512, 320, 384, 320)
SLICE = tuple((768 - rows) // 4 for rows in DIRECT)
DELTA = (0, -1, 1, 2)

FIRST = (
    ((("own_s", 3), ("pair", 1)), ((0, 0), (0, 1))),
    ((("share", 2), ("share", 3), ("rows", 1)), ((1, 0), (1, 1))),
)
FOURS = (
    (
        (
            ("across", 0, 0), ("own_w", 1, 2), ("codes",), ("relay", 2), ("pair", 2), ("rows", 2), ("relay", 3), ("columns", 2),
            ("pair", 3), ("share", 4),
        ),
        ((0, 2), (1, 2), (2, 0), (2, 1)),
    ),
    ((("share", 5), ("far", 0), ("rows", 3)), ((2, 2), (3, 0), (3, 1), (3, 2))),
    (
        (("across", 0, 1), ("own_w", 1, 3), ("pair", 4), ("columns", 3), ("relay", 4)),
        ((0, 3), (1, 3), (2, 3), (3, 3)),
    ),
    ((("across", 1, 0), ("rows", 4), ("relay", 5)), ((4, 0), (4, 1), (4, 2), (4, 3))),
    ((("pair", 5), ("far", 1), ("share", 6), ("columns", 4)), ((0, 4), (1, 4), (2, 4), (3, 4))),
    ((("share", 7), ("rows", 5)), ((4, 4), (5, 0), (5, 1), (5, 2))),
)
EIGHTS = (
    (
        (("across", 1, 1), ("relay", 6), ("columns", 5), ("pair", 6)),
        ((5, 3), (5, 4), (0, 5), (1, 5), (2, 5), (3, 5), (4, 5), (5, 5)),
    ),
    (
        (("relay", 7), ("rows", 6), ("columns", 6), ("pair", 7)),
        ((6, 0), (6, 1), (6, 2), (6, 3), (6, 4), (6, 5), (0, 6), (1, 6)),
    ),
    ((("rows", 7),), ((2, 6), (3, 6), (4, 6), (5, 6), (6, 6), (7, 0), (7, 1), (7, 2))),
    ((("columns", 7),), ((7, 3), (7, 4), (7, 5), (7, 6), (0, 7), (1, 7), (2, 7), (3, 7))),
)
LAST = (((("early",),), ((4, 7), (5, 7), (6, 7), (7, 7))),)


class Numbers:
    def __init__(self):
        self.known = {}

    def __call__(self, *name):
        return self.known.setdefault(name, len(self.known))


def encode_kernel(
    lengths_ref, hidden_ref, dense_ref, b_ref, gain_ref, bias_ref, weight_ref, vbias_ref, terms_ref,
    out_ref, sheet_out_ref,
    hid, den, states, weights, tops, pooled, landed, codes, lows, sheet, boxes, batch_in, vocab_out, vec,
    local_sem, send_sem, recv_sem,
):
    b, v = lax.axis_index("batch"), lax.axis_index("vocab")
    y, c = b // 2, b % 2
    x, z = v // 4, v % 4
    sign = 1 - 2 * c
    number = Numbers()
    started = []

    def device(dx=0, dy=0, dz=0, flip=0):
        core = 1 - c if flip else c
        return (2 * ((y + dy + 4) % 4) + core, 4 * ((x + dx + 4) % 4) + (z + dz + 4) % 4)

    def copy(name, source, target, to):
        i = number(*name)
        assert i < MESSAGES
        return pltpu.make_async_remote_copy(
            src_ref=source, dst_ref=target, send_sem=send_sem.at[i], recv_sem=recv_sem.at[i],
            device_id=to, device_id_type=MESH,
        )

    def send(name, source, target, to):
        copy(name, source, target, to).start()
        if name not in started:
            started.append(name)

    waited = []

    def once(name, act):
        if name not in waited:
            waited.append(name)
            act()

    def got(name, region):
        copy(name, region, region, device(flip=1)).wait_recv()

    def y_rows(j, k):
        return pl.ds(pl.multiple_of(DIRECT[j] + SLICE[j] * ((y + k + 4) % 4), 16), SLICE[j])

    def kind_rows(kind, j):
        return y_rows(j, 0) if kind == 0 else pl.ds(0, DIRECT[j])

    def by_core(j, act):
        if j:
            act(0, 256)
        else:
            pl.when(c == 0)(lambda: act(0, 256))
            pl.when(c == 1)(lambda: act(128, 128))

    wide_first = pl.multiple_of(c * (BLOCK - WIDE), LANES)
    load_h = pltpu.make_async_copy(hidden_ref, hid, local_sem.at[0])
    load_d = pltpu.make_async_copy(dense_ref, den, local_sem.at[1])
    load_w = [
        pltpu.make_async_copy(weight_ref.at[:, pl.ds(pl.multiple_of(wide_first + PIECE * i, LANES), PIECE)], weights.at[i], local_sem.at[2 + i])
        for i in range(2)
    ]
    load_d.start()
    load_h.start()
    for load in load_w:
        load.start()
    barrier = pltpu.get_barrier_semaphore()
    friends = [((b + d) % 8, v) for d in range(1, 8)] + [(b, (v + d) % 16) for d in range(1, 16)]
    friends += [device(dx, 0, 0, 1) for dx in range(1, 4)]
    for friend in friends:
        pl.semaphore_signal(barrier, inc=1, device_id=friend, device_id_type=MESH)

    def send_own_w(kind, j):
        def act(first, width):
            for side, dx in ((0, 1), (1, -1)):
                send(
                    ("x", kind, j, side),
                    weights.at[j // 2, kind_rows(kind, j), pl.ds(256 * (j % 2) + first, width)],
                    weights.at[2 + j, kind_rows(kind, j), pl.ds(256 * side + first, width)],
                    device(dx=dx),
                )

        by_core(j, act)

    def got_own_w(kind, j):
        def act(first, width):
            for side in range(2):
                got(("x", kind, j, side), weights.at[2 + j, kind_rows(kind, j), pl.ds(256 * side + first, width)])

        once(("x", kind, j), lambda: by_core(j, act))

    def fwd_w(kind, i):
        for j in (2 * i, 2 * i + 1):
            got_own_w(kind, j)

            def act(first, width):
                source = weights.at[2 + j, kind_rows(kind, j), pl.ds(pl.multiple_of(256 * c + first, LANES), width)]
                target = weights.at[6 + i, kind_rows(kind, j), pl.ds(256 * (j % 2) + first, width)]
                send(("xf", kind, j), source, target, device(dx=sign))

            by_core(j, act)

    def got_fwd_w(kind, i):
        for j in (2 * i, 2 * i + 1):
            by_core(j, lambda first, width: got(("xf", kind, j), weights.at[6 + i, kind_rows(kind, j), pl.ds(256 * (j % 2) + first, width)]))

    def strips(m):
        return ((m - 2, 0), (m - 2, 256)) if m < 6 else ((2 * m - 12, 0), (2 * m - 11, 256))

    def share_w(m):
        got_own_w(0, m - 2) if m < 6 else got_fwd_w(0, m - 6)
        for j, at in strips(m):
            def act(first, width):
                piece = weights.at[m, y_rows(j, 0), pl.ds(at + first, width)]
                for side, dy in ((0, 1), (1, -1)):
                    send(("y", m, at, side), piece, piece, device(dy=dy))

            by_core(j, act)

    def relay_w(m):
        for j, at in strips(m):
            def act(first, width):
                got(("y", m, at, 0), weights.at[m, y_rows(j, -1), pl.ds(at + first, width)])
                got(("y", m, at, 1), weights.at[m, y_rows(j, 1), pl.ds(at + first, width)])
                piece = weights.at[m, y_rows(j, -sign), pl.ds(at + first, width)]
                send(("yf", m, at), piece, piece, device(dy=sign))

            by_core(j, act)

    def ready_w(m):
        for j, at in strips(m):
            by_core(j, lambda first, width: got(("yf", m, at), weights.at[m, y_rows(j, 2), pl.ds(at + first, width)]))
        got_own_w(1, m - 2) if m < 6 else got_fwd_w(1, m - 6)

    def send_own_s(q):
        for side, dz in ((0, 1), (1, -1)):
            send(("z", q, side), states.at[0, pl.ds(128 * q, 128)], states.at[2 + q, pl.ds(128 * side, 128)], device(dz=dz))

    def got_own_s(q):
        def act():
            for side in range(2):
                got(("z", q, side), states.at[2 + q, pl.ds(128 * side, 128)])

        once(("z", q), act)

    def fwd_s(h):
        for q in (2 * h, 2 * h + 1):
            got_own_s(q)
            source = states.at[2 + q, pl.ds(pl.multiple_of(128 * c, 128), 128)]
            send(("zf", q), source, states.at[6 + h, pl.ds(128 * (q % 2), 128)], device(dz=sign))

    def got_fwd_s(h):
        for q in (2 * h, 2 * h + 1):
            got(("zf", q), states.at[6 + h, pl.ds(128 * (q % 2), 128)])

    def pair_s(k):
        if k >= 6:
            got_fwd_s(k - 6)
        elif k >= 2:
            got_own_s(k - 2)
        if k == 1:
            send(("d", k), states.at[0], states.at[1], device(flip=1))
        else:
            send(("d", k), states.at[k, pl.ds(0, 256)], states.at[k, pl.ds(256, 256)], device(flip=1))

    def paired_s(k):
        got(("d", k), states.at[1] if k == 1 else states.at[k, pl.ds(256, 256)])

    gain, shift, offset = gain_ref[...].reshape(1, -1), bias_ref[...].reshape(1, -1), b_ref[...].reshape(1, -1)

    def head(q, first):
        pre = jnp.dot(hid[128 * q:128 * q + 128, :], den[...], preferred_element_type=jnp.float32) + offset
        act = 0.5 * pre * (1.0 + lax.erf(pre * (0.5 ** 0.5)))
        centered = act - jnp.mean(act, axis=-1, keepdims=True)
        spread = jnp.mean(centered * centered, axis=-1, keepdims=True)
        normed = centered * lax.rsqrt(spread + 1e-06) * gain + shift
        if q % 2 == 0:
            first = normed[0:1, :]
        places = 128 * (q % 2) + lax.broadcasted_iota(jnp.int32, normed.shape, 0)
        normed = jnp.where(places < lengths_ref[2 * v + q // 2], normed, first)
        states[0, 128 * q:128 * q + 128, :] = normed.astype(jnp.bfloat16)
        return first

    load_d.wait()
    load_h.wait()
    first = head(0, None)
    for load in load_w:
        load.wait()
    pl.semaphore_wait(barrier, len(friends))
    for kind, j in ((0, 0), (0, 1), (1, 0), (0, 2), (0, 3), (1, 1)):
        send_own_w(kind, j)
    send_own_s(0)
    for q in range(1, 4):
        first = head(q, first)
        if q > 1:
            send_own_s(q - 1)

    def find_codes():
        k_row = (lax.broadcasted_iota(jnp.int32, (1, K), 1) + 1).astype(jnp.float32)
        j_col = lax.broadcasted_iota(jnp.int32, (16, K), 0)
        o_col = lax.broadcasted_iota(jnp.int32, (LANES, K), 0)
        start = BLOCK * v
        for p in range(32):
            t = terms_ref[p:p + 1, :]
            rel = t - start
            group = jnp.where((t >= 0) & (rel >= 0), rel // LANES, 99)
            one = jnp.where(j_col == group, k_row, 0.0).astype(jnp.bfloat16)
            two = jnp.where(o_col == t % LANES, 1.0, 0.0).astype(jnp.bfloat16)
            found = lax.dot_general(one, two, (((1,), (1,)), ((), ())), preferred_element_type=jnp.float32).astype(jnp.int32)
            codes[:, p, :] = jnp.where(found > 0, p * K + found - 1, BIG)
        lane = lax.broadcasted_iota(jnp.int32, (32, LANES), 1)
        row = lax.broadcasted_iota(jnp.int32, (32, LANES), 0)
        sheet[...] = jnp.zeros_like(sheet)
        last = jnp.full((1, LANES), -1, jnp.int32)
        for slot in range(LIMIT):
            low = jnp.full((32, LANES), BIG, jnp.int32)
            for j in range(15):
                code = codes[j]
                low = jnp.minimum(low, jnp.where(code > last, code, BIG))
            low = jnp.min(low, axis=0, keepdims=True)
            key = jnp.zeros((32, LANES), jnp.int32)
            for j in range(15):
                hit = (codes[j] == low) & (low < BIG)
                key = key + jnp.where(hit, (32 * b + row) * VOCAB_PADDED + start + j * LANES + lane + 1, 0)
            sheet[8 + slot:9 + slot, :] = (jnp.sum(key, axis=0, keepdims=True) - 1).astype(jnp.float32)
            lows[slot:slot + 1, :] = low
            last = low

    back = (0, 2, 1, 3)

    def pool(slots):
        for r in range(4):
            for h in range(2):
                row = 2 * ((z + DELTA[r] + 4) % 4) + h
                for cc in range(2):
                    if r == 0:
                        parts = ((cc, 2 * h), (cc, 2 * h + 1))
                    elif r == 3:
                        parts = ((6 + h, 2 * cc), (6 + h, 2 * cc + 1))
                    else:
                        parts = ((2 + 2 * h, 2 * cc + r - 1), (3 + 2 * h, 2 * cc + r - 1))
                    for m in range(8):
                        slot = (0, 0, 1, 1, 1, 1, 3, 3)[m]
                        if slot not in slots:
                            continue
                        (k0, g0), (k1, g1) = parts
                        best = jnp.max(jnp.maximum(tops[m, k0, g0], tops[m, k1, g1]), axis=0, keepdims=True)
                        if slot == 1:
                            for i in range(2):
                                pooled[1 + i, cc, pl.ds(row, 1), 256 * (m - 2):256 * (m - 1)] = best[:, 256 * i:256 * i + 256]
                        else:
                            pooled[slot, cc, pl.ds(row, 1), PIECE * (m % 2):PIECE * (m % 2) + PIECE] = best

    def swap(slot):
        for cc in range(2):
            if (slot, cc) != (0, 0):
                send(("e", slot, cc), pooled.at[slot, cc], landed.at[cc, back[slot]], device(dx=DELTA[slot], flip=cc))

    def early():
        pool((0, 1))
        for slot in (1, 2, 0):
            swap(slot)

    acts = {
        "own_s": send_own_s, "own_w": send_own_w, "pair": pair_s, "rows": paired_s, "far": fwd_s,
        "share": share_w, "relay": relay_w, "columns": ready_w, "across": fwd_w, "codes": find_codes, "early": early,
    }

    def handle(todo):
        for name, *values in todo:
            acts[name](*values)

    def multiply(k, m):
        d = jnp.dot(states[k], weights[m], preferred_element_type=jnp.float32)
        tops[m, k] = jnp.max(d.reshape(4, 16, 8, PIECE), axis=1)

    def straight(table):
        for todo, pairs in table:
            handle(todo)
            for k, m in pairs:
                multiply(k, m)

    def looped(table):
        def step(n, _):
            for at, (todo, _) in enumerate(table):
                pl.when(n == at)(lambda: handle(todo))
            for part in range(len(table[0][1])):
                k, m = (
                    sum(jnp.where(n == at, pairs[part][i], 0) for at, (_, pairs) in enumerate(table) if pairs[part][i])
                    for i in range(2)
                )
                multiply(k, m)
            return 0

        lax.fori_loop(0, len(table), step, 0)

    straight(FIRST)
    looped(FOURS)
    looped(EIGHTS)
    straight(LAST)
    pool((3,))
    swap(3)
    landed[0, 0] = pooled[0, 0]

    def shape_of(name, width):
        if name[0] in ("x", "xf"):
            return weights.at[2, pl.ds(0, DIRECT[name[2]] if name[1] else SLICE[name[2]]), pl.ds(0, width)]
        if name[0] in ("y", "yf"):
            return weights.at[2, pl.ds(0, SLICE[dict((at, j) for j, at in strips(name[1]))[name[2]]]), pl.ds(0, width)]
        return {
            "z": states.at[0, pl.ds(0, 128)],
            "zf": states.at[0, pl.ds(0, 128)],
            "d": states.at[0] if name[-1] == 1 else states.at[0, pl.ds(0, 256)],
            "e": pooled.at[0, 0],
            "pb": boxes.at[pl.ds(0, 7)],
            "pv": vocab_out.at[pl.ds(0, 15)],
        }[name[0]]

    def quarter_of(name):
        if name[0] in ("x", "xf"):
            return name[2]
        if name[0] in ("y", "yf"):
            return dict((at, j) for j, at in strips(name[1]))[name[2]]
        return 1

    def leave(name):
        by_core(quarter_of(name), lambda first, width: copy(name, shape_of(name, width), shape_of(name, width), device(flip=1)).wait_send())

    for name in [name for name in started if name[0] != "e"]:
        leave(name)
        started.remove(name)
    bias = vbias_ref[...].astype(jnp.float32).reshape(1, -1)
    columns = BLOCK * v + lax.broadcasted_iota(jnp.int32, (8, BLOCK), 1)
    for slot in (0, 1, 2, 3):
        for cc in range(2):
            if (slot, cc) != (0, 0):
                got(("e", back[slot], cc), landed.at[cc, slot])
        raw = jnp.concatenate([landed[c, slot], landed[1 - c, slot][:, 2 * WIDE - BLOCK:]], axis=1) + bias
        done = jnp.where(columns < VOCAB, jnp.log1p(jnp.maximum(raw, 0.0)), 0.0)
        vec[pl.ds(pl.multiple_of(8 * ((x + DELTA[slot] + 4) % 4), 8), 8), :] = done

    for slot in range(LIMIT):
        low = lows[slot:slot + 1, :]
        weight = jnp.zeros((32, LANES), jnp.float32)
        for j in range(15):
            hit = (codes[j] == low) & (low < BIG)
            weight = weight + jnp.where(hit, vec[:, j * LANES:(j + 1) * LANES], 0.0)
        sheet[slot:slot + 1, :] = jnp.sum(weight, axis=0, keepdims=True)
    store = pltpu.make_async_copy(vec, out_ref, local_sem.at[4])
    store.start()
    boxes[...] = jnp.transpose(sheet[...]).reshape(8, 16, LANES)
    for d in range(1, 8):
        to = (b + d) % 8
        send(("pb",), boxes.at[to], batch_in.at[b], (to, v))
    batch_in[b] = boxes[b]
    got(("pb",), batch_in.at[pl.ds(0, 7)])
    for origin in range(8):
        vocab_out[:, origin, :] = batch_in[origin]
    for d in range(1, 16):
        to = (v + d) % 16
        send(("pv",), vocab_out.at[to], sheet_out_ref.at[v], (b, to))
    keep = pltpu.make_async_copy(vocab_out.at[v], sheet_out_ref.at[v], local_sem.at[5])
    keep.start()
    got(("pv",), sheet_out_ref.at[pl.ds(0, 15)])

    store.wait()
    keep.wait()
    for name in started:
        leave(name)


MESSAGES = 89


def encode(hidden, dense_w, dense_b, norm_gain, norm_bias, vocabulary_weight, vocabulary_bias, lengths, term_ids):
    anywhere = pl.BlockSpec(memory_space=pl.ANY)
    vmem = pl.BlockSpec(memory_space=pltpu.VMEM)
    smem = pl.BlockSpec(memory_space=pltpu.SMEM)
    return pl.pallas_call(
        encode_kernel,
        in_specs=[smem, anywhere, anywhere, vmem, vmem, vmem, anywhere, vmem, vmem],
        out_specs=[anywhere, anywhere],
        out_shape=[
            jax.ShapeDtypeStruct((32, BLOCK), jnp.float32),
            jax.ShapeDtypeStruct((16, 8, LANES), jnp.float32),
        ],
        scratch_shapes=[
            pltpu.VMEM((512, 768), jnp.bfloat16),
            pltpu.VMEM((768, 768), jnp.bfloat16),
            pltpu.VMEM((8, 512, 768), jnp.bfloat16),
            pltpu.VMEM((8, 768, PIECE), jnp.bfloat16),
            pltpu.VMEM((8, 8, 4, 8, PIECE), jnp.float32),
            pltpu.VMEM((4, 2, 8, WIDE), jnp.float32),
            pltpu.VMEM((2, 4, 8, WIDE), jnp.float32),
            pltpu.VMEM((16, 32, LANES), jnp.int32),
            pltpu.VMEM((8, LANES), jnp.int32),
            pltpu.VMEM((LANES, LANES), jnp.float32),
            pltpu.VMEM((8, 16, LANES), jnp.float32),
            pltpu.VMEM((8, 16, LANES), jnp.float32),
            pltpu.VMEM((16, 8, LANES), jnp.float32),
            pltpu.VMEM((32, BLOCK), jnp.float32),
            pltpu.SemaphoreType.DMA((6,)),
            pltpu.SemaphoreType.DMA((MESSAGES,)),
            pltpu.SemaphoreType.DMA((MESSAGES,)),
        ],
        compiler_params=pltpu.CompilerParams(collective_id=0, has_side_effects=True, vmem_limit_bytes=56 * 2**20),
    )(lengths, hidden, dense_w, dense_b, norm_gain, norm_bias, vocabulary_weight, vocabulary_bias, term_ids)


def finish_kernel(vectors_ref, sheet_ref, out_ref, out_w_ref, out_k_ref, rows):
    out_ref[...] = vectors_ref[...]
    for origin in range(16):
        rows[:, origin, :] = sheet_ref[origin]
    result = jnp.transpose(rows[...].reshape(LANES, LANES))
    out_w_ref[:, 0, :] = result[0:LIMIT]
    out_k_ref[:, 0, :] = result[8:8 + LIMIT].astype(jnp.int32)


def finish(vectors, sheet):
    vmem = pl.BlockSpec(memory_space=pltpu.VMEM)
    return pl.pallas_call(
        finish_kernel,
        in_specs=[vmem, vmem],
        out_specs=[vmem, vmem, vmem],
        out_shape=[
            jax.ShapeDtypeStruct(vectors.shape, jnp.float32),
            jax.ShapeDtypeStruct((LIMIT, 1, LANES), jnp.float32),
            jax.ShapeDtypeStruct((LIMIT, 1, LANES), jnp.int32),
        ],
        scratch_shapes=[pltpu.VMEM((8, 16, LANES), jnp.float32)],
    )(vectors, sheet)


def local(hidden, dense_w, dense_b, norm_gain, norm_bias, vocabulary_weight, vocabulary_bias, lengths, term_ids):
    vectors, sheet = encode(
        hidden, dense_w, dense_b, norm_gain, norm_bias, vocabulary_weight, vocabulary_bias, lengths, term_ids
    )
    vectors, weights, keys = finish(vectors, sheet)
    return vectors, jnp.swapaxes(weights, 0, 1), jnp.swapaxes(keys, 0, 1)


def solution(mesh):
    in_specs = (
        P(("batch", "vocab"), None), P(), P(), P(), P(),
        P(None, "vocab"), P("vocab"), P("batch"), P("batch", None),
    )
    out_specs = (P("batch", "vocab"), P(("batch", "vocab"), None, None), P(("batch", "vocab"), None, None))
    return jax.shard_map(local, mesh=mesh, in_specs=in_specs, out_specs=out_specs, check_vma=False)
```

```python
import jax
import jax.numpy as jnp
from jax import lax
from jax.experimental import pallas as pl
from jax.experimental.pallas import tpu as pltpu
from jax.sharding import PartitionSpec as P

VOCAB = 30522
VOCAB_PADDED = 30720
K = 128
LIMIT = 5
LANES = 128
BIG = 1 << 20
MESH = pl.DeviceIdType.MESH
BLOCK = 1920
WIDE = 1024
PIECE = 512
DIRECT = (512, 320, 384, 320)
SLICE = tuple((768 - rows) // 4 for rows in DIRECT)
DELTA = (0, -1, 1, 2)

FIRST = (
    ((("own_s", 3), ("pair", 1)), ((0, 0), (0, 1))),
    ((("share", 2), ("share", 3), ("rows", 1)), ((1, 0), (1, 1))),
)
FOURS = (
    (
        (
            ("across", 0, 0), ("own_w", 1, 2), ("codes",), ("relay", 2), ("pair", 2), ("rows", 2), ("relay", 3), ("columns", 2),
            ("pair", 3), ("share", 4),
        ),
        ((0, 2), (1, 2), (2, 0), (2, 1)),
    ),
    ((("share", 5), ("far", 0), ("rows", 3)), ((2, 2), (3, 0), (3, 1), (3, 2))),
    (
        (("across", 0, 1), ("own_w", 1, 3), ("pair", 4), ("columns", 3), ("relay", 4)),
        ((0, 3), (1, 3), (2, 3), (3, 3)),
    ),
    ((("across", 1, 0), ("rows", 4), ("relay", 5)), ((4, 0), (4, 1), (4, 2), (4, 3))),
    ((("pair", 5), ("far", 1), ("share", 6), ("columns", 4)), ((0, 4), (1, 4), (2, 4), (3, 4))),
    ((("share", 7), ("rows", 5)), ((4, 4), (5, 0), (5, 1), (5, 2))),
)
EIGHTS = (
    (
        (("across", 1, 1), ("relay", 6), ("columns", 5), ("pair", 6)),
        ((5, 3), (5, 4), (0, 5), (1, 5), (2, 5), (3, 5), (4, 5), (5, 5)),
    ),
    (
        (("relay", 7), ("rows", 6), ("columns", 6), ("pair", 7)),
        ((6, 0), (6, 1), (6, 2), (6, 3), (6, 4), (6, 5), (0, 6), (1, 6)),
    ),
    ((("rows", 7),), ((2, 6), (3, 6), (4, 6), (5, 6), (6, 6), (7, 0), (7, 1), (7, 2))),
    ((("columns", 7),), ((7, 3), (7, 4), (7, 5), (7, 6), (0, 7), (1, 7), (2, 7), (3, 7))),
)
LAST = (((("early",),), ((4, 7), (5, 7), (6, 7), (7, 7))),)


class Numbers:
    def __init__(self):
        self.known = {}

    def __call__(self, *name):
        return self.known.setdefault(name, len(self.known))


def encode_kernel(
    lengths_ref, hidden_ref, dense_ref, b_ref, gain_ref, bias_ref, weight_ref, vbias_ref, terms_ref,
    out_ref, sheet_out_ref,
    hid, den, states, weights, tops, pooled, landed, codes, lows, sheet, boxes, batch_in, vocab_out, vec,
    local_sem, send_sem, recv_sem,
):
    b, v = lax.axis_index("batch"), lax.axis_index("vocab")
    y, c = b // 2, b % 2
    x, z = v // 4, v % 4
    sign = 1 - 2 * c
    number = Numbers()

    def group_of(name):
        if name[0] in ("x", "xf"):
            quarter = name[2]
        elif name[0] in ("y", "yf"):
            quarter = name[1] - 2 if name[1] < 6 else 2 * name[1] - 12 + name[2] // 256
        else:
            return {"z": 0, "zf": 0, "d": 0, "e": 3, "pb": 4, "pv": 5}[name[0]]
        return 2 if quarter else 1


    def device(dx=0, dy=0, dz=0, flip=0):
        core = 1 - c if flip else c
        return (2 * ((y + dy + 4) % 4) + core, 4 * ((x + dx + 4) % 4) + (z + dz + 4) % 4)

    def copy(name, source, target, to):
        i = number(*name)
        assert i < MESSAGES
        return pltpu.make_async_remote_copy(
            src_ref=source, dst_ref=target, send_sem=send_sem.at[group_of(name)], recv_sem=recv_sem.at[i],
            device_id=to, device_id_type=MESH,
        )

    def send(name, source, target, to):
        copy(name, source, target, to).start()

    waited = []

    def once(name, act):
        if name not in waited:
            waited.append(name)
            act()

    def got(name, region):
        copy(name, region, region, device(flip=1)).wait_recv()

    def y_rows(j, k):
        return pl.ds(pl.multiple_of(DIRECT[j] + SLICE[j] * ((y + k + 4) % 4), 16), SLICE[j])

    def kind_rows(kind, j):
        return y_rows(j, 0) if kind == 0 else pl.ds(0, DIRECT[j])

    def by_core(j, act):
        if j:
            act(0, 256)
        else:
            pl.when(c == 0)(lambda: act(0, 256))
            pl.when(c == 1)(lambda: act(128, 128))

    wide_first = pl.multiple_of(c * (BLOCK - WIDE), LANES)
    load_h = pltpu.make_async_copy(hidden_ref, hid, local_sem.at[0])
    load_d = pltpu.make_async_copy(dense_ref, den, local_sem.at[1])
    load_w = [
        pltpu.make_async_copy(weight_ref.at[:, pl.ds(pl.multiple_of(wide_first + PIECE * i, LANES), PIECE)], weights.at[i], local_sem.at[2 + i])
        for i in range(2)
    ]
    load_d.start()
    load_h.start()
    for load in load_w:
        load.start()
    barrier = pltpu.get_barrier_semaphore()
    friends = [((b + d) % 8, v) for d in range(1, 8)] + [(b, (v + d) % 16) for d in range(1, 16)]
    friends += [device(dx, 0, 0, 1) for dx in range(1, 4)]
    for friend in friends:
        pl.semaphore_signal(barrier, inc=1, device_id=friend, device_id_type=MESH)

    def send_own_w(kind, j):
        def act(first, width):
            for side, dx in ((0, 1), (1, -1)):
                send(
                    ("x", kind, j),
                    weights.at[j // 2, kind_rows(kind, j), pl.ds(256 * (j % 2) + first, width)],
                    weights.at[2 + j, kind_rows(kind, j), pl.ds(256 * side + first, width)],
                    device(dx=dx),
                )

        by_core(j, act)

    def got_own_w(kind, j):
        def act(first, width):
            got(("x", kind, j), weights.at[2 + j, kind_rows(kind, j), pl.ds(0, 2 * width)])

        once(("x", kind, j), lambda: by_core(j, act))

    def fwd_w(kind, i):
        for j in (2 * i, 2 * i + 1):
            got_own_w(kind, j)

            def act(first, width):
                source = weights.at[2 + j, kind_rows(kind, j), pl.ds(pl.multiple_of(256 * c + first, LANES), width)]
                target = weights.at[6 + i, kind_rows(kind, j), pl.ds(256 * (j % 2) + first, width)]
                send(("xf", kind, j), source, target, device(dx=sign))

            by_core(j, act)

    def got_fwd_w(kind, i):
        for j in (2 * i, 2 * i + 1):
            by_core(j, lambda first, width: got(("xf", kind, j), weights.at[6 + i, kind_rows(kind, j), pl.ds(256 * (j % 2) + first, width)]))

    def strips(m):
        return ((m - 2, 0), (m - 2, 256)) if m < 6 else ((2 * m - 12, 0), (2 * m - 11, 256))

    def share_w(m):
        got_own_w(0, m - 2) if m < 6 else got_fwd_w(0, m - 6)
        for j, at in strips(m):
            def act(first, width):
                piece = weights.at[m, y_rows(j, 0), pl.ds(at + first, width)]
                for side, dy in ((0, 1), (1, -1)):
                    send(("y", m, at if m >= 6 else 0), piece, piece, device(dy=dy))

            by_core(j, act)

    def together(m):
        return ((m - 2, 0, 2),) if m < 6 else ((2 * m - 12, 0, 1), (2 * m - 11, 256, 1))

    def relay_w(m):
        for j, at, n in together(m):
            by_core(j, lambda first, width: got(("y", m, at), weights.at[m, pl.ds(0, 2 * SLICE[j]), pl.ds(at, n * width)]))
        for j, at in strips(m):
            def act(first, width):
                piece = weights.at[m, y_rows(j, -sign), pl.ds(at + first, width)]
                send(("yf", m, at if m >= 6 else 0), piece, piece, device(dy=sign))

            by_core(j, act)

    def ready_w(m):
        for j, at, n in together(m):
            by_core(j, lambda first, width: got(("yf", m, at), weights.at[m, pl.ds(0, SLICE[j]), pl.ds(at, n * width)]))
        got_own_w(1, m - 2) if m < 6 else got_fwd_w(1, m - 6)

    def send_own_s(q):
        for side, dz in ((0, 1), (1, -1)):
            send(("z", q), states.at[0, pl.ds(128 * q, 128)], states.at[2 + q, pl.ds(128 * side, 128)], device(dz=dz))

    def got_own_s(q):
        def act():
            got(("z", q), states.at[2 + q, pl.ds(0, 256)])

        once(("z", q), act)

    def fwd_s(h):
        for q in (2 * h, 2 * h + 1):
            got_own_s(q)
            source = states.at[2 + q, pl.ds(pl.multiple_of(128 * c, 128), 128)]
            send(("zf", h), source, states.at[6 + h, pl.ds(128 * (q % 2), 128)], device(dz=sign))

    def got_fwd_s(h):
        got(("zf", h), states.at[6 + h, pl.ds(0, 256)])

    def pair_s(k):
        if k >= 6:
            got_fwd_s(k - 6)
        elif k >= 2:
            got_own_s(k - 2)
        if k == 1:
            send(("d", k), states.at[0], states.at[1], device(flip=1))
        else:
            send(("d", k), states.at[k, pl.ds(0, 256)], states.at[k, pl.ds(256, 256)], device(flip=1))

    def paired_s(k):
        got(("d", k), states.at[1] if k == 1 else states.at[k, pl.ds(256, 256)])

    gain, shift, offset = gain_ref[...].reshape(1, -1), bias_ref[...].reshape(1, -1), b_ref[...].reshape(1, -1)

    def head(q, first):
        pre = jnp.dot(hid[128 * q:128 * q + 128, :], den[...], preferred_element_type=jnp.float32) + offset
        act = 0.5 * pre * (1.0 + lax.erf(pre * (0.5 ** 0.5)))
        centered = act - jnp.mean(act, axis=-1, keepdims=True)
        spread = jnp.mean(centered * centered, axis=-1, keepdims=True)
        normed = centered * lax.rsqrt(spread + 1e-06) * gain + shift
        if q % 2 == 0:
            first = normed[0:1, :]
        places = 128 * (q % 2) + lax.broadcasted_iota(jnp.int32, normed.shape, 0)
        normed = jnp.where(places < lengths_ref[2 * v + q // 2], normed, first)
        states[0, 128 * q:128 * q + 128, :] = normed.astype(jnp.bfloat16)
        return first

    load_d.wait()
    load_h.wait()
    first = head(0, None)
    for load in load_w:
        load.wait()
    pl.semaphore_wait(barrier, len(friends))
    for kind, j in ((0, 0), (0, 1), (1, 0), (0, 2), (0, 3), (1, 1)):
        send_own_w(kind, j)
    send_own_s(0)
    for q in range(1, 4):
        first = head(q, first)
        if q > 1:
            send_own_s(q - 1)

    def find_codes():
        k_row = (lax.broadcasted_iota(jnp.int32, (1, K), 1) + 1).astype(jnp.float32)
        j_col = lax.broadcasted_iota(jnp.int32, (16, K), 0)
        o_col = lax.broadcasted_iota(jnp.int32, (LANES, K), 0)
        start = BLOCK * v
        for p in range(32):
            t = terms_ref[p:p + 1, :]
            rel = t - start
            group = jnp.where((t >= 0) & (rel >= 0), rel // LANES, 99)
            one = jnp.where(j_col == group, k_row, 0.0).astype(jnp.bfloat16)
            two = jnp.where(o_col == t % LANES, 1.0, 0.0).astype(jnp.bfloat16)
            found = lax.dot_general(one, two, (((1,), (1,)), ((), ())), preferred_element_type=jnp.float32).astype(jnp.int32)
            codes[:, p, :] = jnp.where(found > 0, p * K + found - 1, BIG)
        lane = lax.broadcasted_iota(jnp.int32, (32, LANES), 1)
        row = lax.broadcasted_iota(jnp.int32, (32, LANES), 0)
        sheet[...] = jnp.zeros_like(sheet)
        last = jnp.full((1, LANES), -1, jnp.int32)
        for slot in range(LIMIT):
            low = jnp.full((32, LANES), BIG, jnp.int32)
            for j in range(15):
                code = codes[j]
                low = jnp.minimum(low, jnp.where(code > last, code, BIG))
            low = jnp.min(low, axis=0, keepdims=True)
            key = jnp.zeros((32, LANES), jnp.int32)
            for j in range(15):
                hit = (codes[j] == low) & (low < BIG)
                key = key + jnp.where(hit, (32 * b + row) * VOCAB_PADDED + start + j * LANES + lane + 1, 0)
            sheet[8 + slot:9 + slot, :] = (jnp.sum(key, axis=0, keepdims=True) - 1).astype(jnp.float32)
            lows[slot:slot + 1, :] = low
            last = low

    back = (0, 2, 1, 3)

    def pool(slots):
        for r in range(4):
            for h in range(2):
                row = 2 * ((z + DELTA[r] + 4) % 4) + h
                for cc in range(2):
                    if r == 0:
                        parts = ((cc, 2 * h), (cc, 2 * h + 1))
                    elif r == 3:
                        parts = ((6 + h, 2 * cc), (6 + h, 2 * cc + 1))
                    else:
                        parts = ((2 + 2 * h, 2 * cc + r - 1), (3 + 2 * h, 2 * cc + r - 1))
                    for m in range(8):
                        slot = (0, 0, 1, 1, 1, 1, 3, 3)[m]
                        if slot not in slots:
                            continue
                        (k0, g0), (k1, g1) = parts
                        best = jnp.max(jnp.maximum(tops[m, k0, g0], tops[m, k1, g1]), axis=0, keepdims=True)
                        if slot == 1:
                            for i in range(2):
                                pooled[1 + i, cc, pl.ds(row, 1), 256 * (m - 2):256 * (m - 1)] = best[:, 256 * i:256 * i + 256]
                        else:
                            pooled[slot, cc, pl.ds(row, 1), PIECE * (m % 2):PIECE * (m % 2) + PIECE] = best

    def swap(slot):
        for cc in range(2):
            if (slot, cc) != (0, 0):
                send(("e", slot, cc), pooled.at[slot, cc], landed.at[cc, back[slot]], device(dx=DELTA[slot], flip=cc))

    def early():
        pool((0, 1))
        for slot in (1, 2, 0):
            swap(slot)

    acts = {
        "own_s": send_own_s, "own_w": send_own_w, "pair": pair_s, "rows": paired_s, "far": fwd_s,
        "share": share_w, "relay": relay_w, "columns": ready_w, "across": fwd_w, "codes": find_codes, "early": early,
    }

    def handle(todo):
        for name, *values in todo:
            acts[name](*values)

    def multiply(k, m):
        d = jnp.dot(states[k], weights[m], preferred_element_type=jnp.float32)
        tops[m, k] = jnp.max(d.reshape(4, 16, 8, PIECE), axis=1)

    def straight(table):
        for todo, pairs in table:
            handle(todo)
            for k, m in pairs:
                multiply(k, m)

    def looped(table):
        def step(n, _):
            for at, (todo, _) in enumerate(table):
                pl.when(n == at)(lambda: handle(todo))
            for part in range(len(table[0][1])):
                k, m = (
                    sum(jnp.where(n == at, pairs[part][i], 0) for at, (_, pairs) in enumerate(table) if pairs[part][i])
                    for i in range(2)
                )
                multiply(k, m)
            return 0

        lax.fori_loop(0, len(table), step, 0)

    straight(FIRST)
    looped(FOURS)
    looped(EIGHTS)
    straight(LAST)
    pool((3,))
    swap(3)
    landed[0, 0] = pooled[0, 0]

    def leave(name, region):
        copy(name, region, region, device(flip=1)).wait_send()

    leave(("z", 0), states.at[pl.ds(0, 7)])
    by_core(0, lambda first, width: leave(("x", 0, 0), weights.at[pl.ds(0, 3), :, pl.ds(0, width)]))
    leave(("x", 0, 1), weights.at[pl.ds(0, 6), :, pl.ds(0, 384)])
    bias = vbias_ref[...].astype(jnp.float32).reshape(1, -1)
    columns = BLOCK * v + lax.broadcasted_iota(jnp.int32, (8, BLOCK), 1)
    for slot in (0, 1, 2, 3):
        for cc in range(2):
            if (slot, cc) != (0, 0):
                got(("e", back[slot], cc), landed.at[cc, slot])
        raw = jnp.concatenate([landed[c, slot], landed[1 - c, slot][:, 2 * WIDE - BLOCK:]], axis=1) + bias
        done = jnp.where(columns < VOCAB, jnp.log1p(jnp.maximum(raw, 0.0)), 0.0)
        vec[pl.ds(pl.multiple_of(8 * ((x + DELTA[slot] + 4) % 4), 8), 8), :] = done

    for slot in range(LIMIT):
        low = lows[slot:slot + 1, :]
        weight = jnp.zeros((32, LANES), jnp.float32)
        for j in range(15):
            hit = (codes[j] == low) & (low < BIG)
            weight = weight + jnp.where(hit, vec[:, j * LANES:(j + 1) * LANES], 0.0)
        sheet[slot:slot + 1, :] = jnp.sum(weight, axis=0, keepdims=True)
    store = pltpu.make_async_copy(vec, out_ref, local_sem.at[4])
    store.start()
    boxes[...] = jnp.transpose(sheet[...]).reshape(8, 16, LANES)
    for d in range(1, 8):
        to = (b + d) % 8
        send(("pb",), boxes.at[to], batch_in.at[b], (to, v))
    batch_in[b] = boxes[b]
    got(("pb",), batch_in.at[pl.ds(0, 7)])
    for origin in range(8):
        vocab_out[:, origin, :] = batch_in[origin]
    for d in range(1, 16):
        to = (v + d) % 16
        send(("pv",), vocab_out.at[to], sheet_out_ref.at[v], (b, to))
    keep = pltpu.make_async_copy(vocab_out.at[v], sheet_out_ref.at[v], local_sem.at[5])
    keep.start()
    got(("pv",), sheet_out_ref.at[pl.ds(0, 15)])

    store.wait()
    keep.wait()
    leave(("e", 0, 1), tops.at[0, pl.ds(0, 7), pl.ds(0, 2)])
    leave(("pb",), boxes.at[pl.ds(0, 7)])
    leave(("pv",), vocab_out.at[pl.ds(0, 15)])


MESSAGES = 54


def encode(hidden, dense_w, dense_b, norm_gain, norm_bias, vocabulary_weight, vocabulary_bias, lengths, term_ids):
    anywhere = pl.BlockSpec(memory_space=pl.ANY)
    vmem = pl.BlockSpec(memory_space=pltpu.VMEM)
    smem = pl.BlockSpec(memory_space=pltpu.SMEM)
    return pl.pallas_call(
        encode_kernel,
        in_specs=[smem, anywhere, anywhere, vmem, vmem, vmem, anywhere, vmem, vmem],
        out_specs=[anywhere, anywhere],
        out_shape=[
            jax.ShapeDtypeStruct((32, BLOCK), jnp.float32),
            jax.ShapeDtypeStruct((16, 8, LANES), jnp.float32),
        ],
        scratch_shapes=[
            pltpu.VMEM((512, 768), jnp.bfloat16),
            pltpu.VMEM((768, 768), jnp.bfloat16),
            pltpu.VMEM((8, 512, 768), jnp.bfloat16),
            pltpu.VMEM((8, 768, PIECE), jnp.bfloat16),
            pltpu.VMEM((8, 8, 4, 8, PIECE), jnp.float32),
            pltpu.VMEM((4, 2, 8, WIDE), jnp.float32),
            pltpu.VMEM((2, 4, 8, WIDE), jnp.float32),
            pltpu.VMEM((16, 32, LANES), jnp.int32),
            pltpu.VMEM((8, LANES), jnp.int32),
            pltpu.VMEM((LANES, LANES), jnp.float32),
            pltpu.VMEM((8, 16, LANES), jnp.float32),
            pltpu.VMEM((8, 16, LANES), jnp.float32),
            pltpu.VMEM((16, 8, LANES), jnp.float32),
            pltpu.VMEM((32, BLOCK), jnp.float32),
            pltpu.SemaphoreType.DMA((6,)),
            pltpu.SemaphoreType.DMA((6,)),
            pltpu.SemaphoreType.DMA((MESSAGES,)),
        ],
        compiler_params=pltpu.CompilerParams(collective_id=0, has_side_effects=True, vmem_limit_bytes=56 * 2**20),
    )(lengths, hidden, dense_w, dense_b, norm_gain, norm_bias, vocabulary_weight, vocabulary_bias, term_ids)


def finish_kernel(vectors_ref, sheet_ref, out_ref, out_w_ref, out_k_ref, rows):
    out_ref[...] = vectors_ref[...]
    for origin in range(16):
        rows[:, origin, :] = sheet_ref[origin]
    result = jnp.transpose(rows[...].reshape(LANES, LANES))
    out_w_ref[:, 0, :] = result[0:LIMIT]
    out_k_ref[:, 0, :] = result[8:8 + LIMIT].astype(jnp.int32)


def finish(vectors, sheet):
    vmem = pl.BlockSpec(memory_space=pltpu.VMEM)
    return pl.pallas_call(
        finish_kernel,
        in_specs=[vmem, vmem],
        out_specs=[vmem, vmem, vmem],
        out_shape=[
            jax.ShapeDtypeStruct(vectors.shape, jnp.float32),
            jax.ShapeDtypeStruct((LIMIT, 1, LANES), jnp.float32),
            jax.ShapeDtypeStruct((LIMIT, 1, LANES), jnp.int32),
        ],
        scratch_shapes=[pltpu.VMEM((8, 16, LANES), jnp.float32)],
    )(vectors, sheet)


def local(hidden, dense_w, dense_b, norm_gain, norm_bias, vocabulary_weight, vocabulary_bias, lengths, term_ids):
    vectors, sheet = encode(
        hidden, dense_w, dense_b, norm_gain, norm_bias, vocabulary_weight, vocabulary_bias, lengths, term_ids
    )
    vectors, weights, keys = finish(vectors, sheet)
    return vectors, jnp.swapaxes(weights, 0, 1), jnp.swapaxes(keys, 0, 1)


def solution(mesh):
    in_specs = (
        P(("batch", "vocab"), None), P(), P(), P(), P(),
        P(None, "vocab"), P("vocab"), P("batch"), P("batch", None),
    )
    out_specs = (P("batch", "vocab"), P(("batch", "vocab"), None, None), P(("batch", "vocab"), None, None))
    return jax.shard_map(local, mesh=mesh, in_specs=in_specs, out_specs=out_specs, check_vma=False)
```

```python
import jax
import jax.numpy as jnp
from jax import lax
from jax.experimental import pallas as pl
from jax.experimental.pallas import tpu as pltpu
from jax.sharding import PartitionSpec as P

VOCAB = 30522
VOCAB_PADDED = 30720
K = 128
LIMIT = 5
LANES = 128
BIG = 1 << 20
MESH = pl.DeviceIdType.MESH
BLOCK = 1920
WIDE = 1024
PIECE = 512
DIRECT = (512, 320, 384, 320)
SLICE = tuple((768 - rows) // 4 for rows in DIRECT)
DELTA = (0, -1, 1, 2)

FIRST = (
    ((("own_s", 3), ("pair", 1)), ((0, 0), (0, 1))),
    ((("share", 2), ("share", 3), ("rows", 1)), ((1, 0), (1, 1))),
)
FOURS = (
    (
        (
            ("across", 0, 0), ("own_w", 1, 2), ("codes",), ("relay", 2), ("pair", 2), ("rows", 2), ("relay", 3), ("columns", 2),
            ("pair", 3), ("share", 4),
        ),
        ((0, 2), (1, 2), (2, 0), (2, 1)),
    ),
    ((("share", 5), ("far", 0), ("rows", 3)), ((2, 2), (3, 0), (3, 1), (3, 2))),
    (
        (("across", 0, 1), ("own_w", 1, 3), ("pair", 4), ("columns", 3), ("relay", 4)),
        ((0, 3), (1, 3), (2, 3), (3, 3)),
    ),
    ((("across", 1, 0), ("rows", 4), ("relay", 5)), ((4, 0), (4, 1), (4, 2), (4, 3))),
    ((("pair", 5), ("far", 1), ("share", 6), ("columns", 4)), ((0, 4), (1, 4), (2, 4), (3, 4))),
    ((("share", 7), ("rows", 5)), ((4, 4), (5, 0), (5, 1), (5, 2))),
)
EIGHTS = (
    (
        (("across", 1, 1), ("relay", 6), ("columns", 5), ("pair", 6)),
        ((5, 3), (5, 4), (0, 5), (1, 5), (2, 5), (3, 5), (4, 5), (5, 5)),
    ),
    (
        (("relay", 7), ("rows", 6), ("columns", 6), ("pair", 7)),
        ((6, 0), (6, 1), (6, 2), (6, 3), (6, 4), (6, 5), (0, 6), (1, 6)),
    ),
    ((("rows", 7),), ((2, 6), (3, 6), (4, 6), (5, 6), (6, 6), (7, 0), (7, 1), (7, 2))),
    ((("columns", 7),), ((7, 3), (7, 4), (7, 5), (7, 6), (0, 7), (1, 7), (2, 7), (3, 7))),
)
LAST = (((("early",),), ((4, 7), (5, 7), (6, 7), (7, 7))),)


class Numbers:
    def __init__(self):
        self.known = {}

    def __call__(self, *name):
        return self.known.setdefault(name, len(self.known))


def encode_kernel(
    lengths_ref, hidden_ref, dense_ref, b_ref, gain_ref, bias_ref, weight_ref, vbias_ref, terms_hbm_ref,
    out_ref, sheet_out_ref,
    hid, den, states, weights, tops, pooled, landed, codes, lows, sheet, boxes, batch_in, vocab_out, vec, terms_ref,
    local_sem, send_sem, recv_sem,
):
    b, v = lax.axis_index("batch"), lax.axis_index("vocab")
    y, c = b // 2, b % 2
    x, z = v // 4, v % 4
    sign = 1 - 2 * c
    number = Numbers()

    def group_of(name):
        if name[0] in ("x", "xf"):
            quarter = name[2]
        elif name[0] in ("y", "yf"):
            quarter = name[1] - 2 if name[1] < 6 else 2 * name[1] - 12 + name[2] // 256
        else:
            return {"z": 0, "zf": 0, "d": 0, "e": 3, "pb": 4, "pv": 5}[name[0]]
        return 2 if quarter else 1


    def device(dx=0, dy=0, dz=0, flip=0):
        core = 1 - c if flip else c
        return (2 * ((y + dy + 4) % 4) + core, 4 * ((x + dx + 4) % 4) + (z + dz + 4) % 4)

    def copy(name, source, target, to):
        i = number(*name)
        assert i < MESSAGES
        return pltpu.make_async_remote_copy(
            src_ref=source, dst_ref=target, send_sem=send_sem.at[group_of(name)], recv_sem=recv_sem.at[i],
            device_id=to, device_id_type=MESH,
        )

    def send(name, source, target, to):
        copy(name, source, target, to).start()

    waited = []

    def once(name, act):
        if name not in waited:
            waited.append(name)
            act()

    def got(name, region):
        copy(name, region, region, device(flip=1)).wait_recv()

    def y_rows(j, k):
        return pl.ds(pl.multiple_of(DIRECT[j] + SLICE[j] * ((y + k + 4) % 4), 16), SLICE[j])

    def kind_rows(kind, j):
        return y_rows(j, 0) if kind == 0 else pl.ds(0, DIRECT[j])

    def by_core(j, act):
        if j:
            act(0, 256)
        else:
            pl.when(c == 0)(lambda: act(0, 256))
            pl.when(c == 1)(lambda: act(128, 128))

    wide_first = pl.multiple_of(c * (BLOCK - WIDE), LANES)
    load_h = pltpu.make_async_copy(hidden_ref, hid, local_sem.at[0])
    load_d = pltpu.make_async_copy(dense_ref, den, local_sem.at[1])
    load_w = [
        pltpu.make_async_copy(weight_ref.at[:, pl.ds(pl.multiple_of(wide_first + PIECE * i, LANES), PIECE)], weights.at[i], local_sem.at[2 + i])
        for i in range(2)
    ]
    load_d.start()
    load_h.start()
    for load in load_w:
        load.start()
    load_t = pltpu.make_async_copy(terms_hbm_ref, terms_ref, local_sem.at[6])
    load_t.start()
    barrier = pltpu.get_barrier_semaphore()
    friends = [((b + d) % 8, v) for d in range(1, 8)] + [(b, (v + d) % 16) for d in range(1, 16)]
    friends += [device(dx, 0, 0, 1) for dx in range(1, 4)]
    for friend in friends:
        pl.semaphore_signal(barrier, inc=1, device_id=friend, device_id_type=MESH)

    def send_own_w(kind, j):
        def act(first, width):
            for side, dx in ((0, 1), (1, -1)):
                send(
                    ("x", kind, j),
                    weights.at[j // 2, kind_rows(kind, j), pl.ds(256 * (j % 2) + first, width)],
                    weights.at[2 + j, kind_rows(kind, j), pl.ds(256 * side + first, width)],
                    device(dx=dx),
                )

        by_core(j, act)

    def got_own_w(kind, j):
        def act(first, width):
            got(("x", kind, j), weights.at[2 + j, kind_rows(kind, j), pl.ds(0, 2 * width)])

        once(("x", kind, j), lambda: by_core(j, act))

    def fwd_w(kind, i):
        for j in (2 * i, 2 * i + 1):
            got_own_w(kind, j)

            def act(first, width):
                source = weights.at[2 + j, kind_rows(kind, j), pl.ds(pl.multiple_of(256 * c + first, LANES), width)]
                target = weights.at[6 + i, kind_rows(kind, j), pl.ds(256 * (j % 2) + first, width)]
                send(("xf", kind, j), source, target, device(dx=sign))

            by_core(j, act)

    def got_fwd_w(kind, i):
        for j in (2 * i, 2 * i + 1):
            by_core(j, lambda first, width: got(("xf", kind, j), weights.at[6 + i, kind_rows(kind, j), pl.ds(256 * (j % 2) + first, width)]))

    def strips(m):
        return ((m - 2, 0), (m - 2, 256)) if m < 6 else ((2 * m - 12, 0), (2 * m - 11, 256))

    def share_w(m):
        got_own_w(0, m - 2) if m < 6 else got_fwd_w(0, m - 6)
        for j, at in strips(m):
            def act(first, width):
                piece = weights.at[m, y_rows(j, 0), pl.ds(at + first, width)]
                for side, dy in ((0, 1), (1, -1)):
                    send(("y", m, at if m >= 6 else 0), piece, piece, device(dy=dy))

            by_core(j, act)

    def together(m):
        return ((m - 2, 0, 2),) if m < 6 else ((2 * m - 12, 0, 1), (2 * m - 11, 256, 1))

    def relay_w(m):
        for j, at, n in together(m):
            by_core(j, lambda first, width: got(("y", m, at), weights.at[m, pl.ds(0, 2 * SLICE[j]), pl.ds(at, n * width)]))
        for j, at in strips(m):
            def act(first, width):
                piece = weights.at[m, y_rows(j, -sign), pl.ds(at + first, width)]
                send(("yf", m, at if m >= 6 else 0), piece, piece, device(dy=sign))

            by_core(j, act)

    def ready_w(m):
        for j, at, n in together(m):
            by_core(j, lambda first, width: got(("yf", m, at), weights.at[m, pl.ds(0, SLICE[j]), pl.ds(at, n * width)]))
        got_own_w(1, m - 2) if m < 6 else got_fwd_w(1, m - 6)

    def send_own_s(q):
        for side, dz in ((0, 1), (1, -1)):
            send(("z", q), states.at[0, pl.ds(128 * q, 128)], states.at[2 + q, pl.ds(128 * side, 128)], device(dz=dz))

    def got_own_s(q):
        def act():
            got(("z", q), states.at[2 + q, pl.ds(0, 256)])

        once(("z", q), act)

    def fwd_s(h):
        for q in (2 * h, 2 * h + 1):
            got_own_s(q)
            source = states.at[2 + q, pl.ds(pl.multiple_of(128 * c, 128), 128)]
            send(("zf", h), source, states.at[6 + h, pl.ds(128 * (q % 2), 128)], device(dz=sign))

    def got_fwd_s(h):
        got(("zf", h), states.at[6 + h, pl.ds(0, 256)])

    def pair_s(k):
        if k >= 6:
            got_fwd_s(k - 6)
        elif k >= 2:
            got_own_s(k - 2)
        if k == 1:
            send(("d", k), states.at[0], states.at[1], device(flip=1))
        else:
            send(("d", k), states.at[k, pl.ds(0, 256)], states.at[k, pl.ds(256, 256)], device(flip=1))

    def paired_s(k):
        got(("d", k), states.at[1] if k == 1 else states.at[k, pl.ds(256, 256)])

    gain, shift, offset = gain_ref[...].reshape(1, -1), bias_ref[...].reshape(1, -1), b_ref[...].reshape(1, -1)

    def head(q, first):
        pre = jnp.dot(hid[128 * q:128 * q + 128, :], den[...], preferred_element_type=jnp.float32) + offset
        act = 0.5 * pre * (1.0 + lax.erf(pre * (0.5 ** 0.5)))
        centered = act - jnp.mean(act, axis=-1, keepdims=True)
        spread = jnp.mean(centered * centered, axis=-1, keepdims=True)
        normed = centered * lax.rsqrt(spread + 1e-06) * gain + shift
        if q % 2 == 0:
            first = normed[0:1, :]
        places = 128 * (q % 2) + lax.broadcasted_iota(jnp.int32, normed.shape, 0)
        normed = jnp.where(places < lengths_ref[2 * v + q // 2], normed, first)
        states[0, 128 * q:128 * q + 128, :] = normed.astype(jnp.bfloat16)
        return first

    load_d.wait()
    load_h.wait()
    first = head(0, None)
    for load in load_w:
        load.wait()
    pl.semaphore_wait(barrier, len(friends))
    for kind, j in ((0, 0), (0, 1), (1, 0), (0, 2), (0, 3), (1, 1)):
        send_own_w(kind, j)
    send_own_s(0)
    for q in range(1, 4):
        first = head(q, first)
        if q > 1:
            send_own_s(q - 1)

    def find_codes():
        load_t.wait()
        k_row = (lax.broadcasted_iota(jnp.int32, (1, K), 1) + 1).astype(jnp.float32)
        j_col = lax.broadcasted_iota(jnp.int32, (16, K), 0)
        o_col = lax.broadcasted_iota(jnp.int32, (LANES, K), 0)
        start = BLOCK * v
        for p in range(32):
            t = terms_ref[p:p + 1, :]
            rel = t - start
            group = jnp.where((t >= 0) & (rel >= 0), rel // LANES, 99)
            one = jnp.where(j_col == group, k_row, 0.0).astype(jnp.bfloat16)
            two = jnp.where(o_col == t % LANES, 1.0, 0.0).astype(jnp.bfloat16)
            found = lax.dot_general(one, two, (((1,), (1,)), ((), ())), preferred_element_type=jnp.float32).astype(jnp.int32)
            codes[:, p, :] = jnp.where(found > 0, p * K + found - 1, BIG)
        lane = lax.broadcasted_iota(jnp.int32, (32, LANES), 1)
        row = lax.broadcasted_iota(jnp.int32, (32, LANES), 0)
        sheet[...] = jnp.zeros_like(sheet)
        last = jnp.full((1, LANES), -1, jnp.int32)
        for slot in range(LIMIT):
            low = jnp.full((32, LANES), BIG, jnp.int32)
            for j in range(15):
                code = codes[j]
                low = jnp.minimum(low, jnp.where(code > last, code, BIG))
            low = jnp.min(low, axis=0, keepdims=True)
            key = jnp.zeros((32, LANES), jnp.int32)
            for j in range(15):
                hit = (codes[j] == low) & (low < BIG)
                key = key + jnp.where(hit, (32 * b + row) * VOCAB_PADDED + start + j * LANES + lane + 1, 0)
            sheet[8 + slot:9 + slot, :] = (jnp.sum(key, axis=0, keepdims=True) - 1).astype(jnp.float32)
            lows[slot:slot + 1, :] = low
            last = low

    back = (0, 2, 1, 3)

    def pool(slots):
        for r in range(4):
            for h in range(2):
                row = 2 * ((z + DELTA[r] + 4) % 4) + h
                for cc in range(2):
                    if r == 0:
                        parts = ((cc, 2 * h), (cc, 2 * h + 1))
                    elif r == 3:
                        parts = ((6 + h, 2 * cc), (6 + h, 2 * cc + 1))
                    else:
                        parts = ((2 + 2 * h, 2 * cc + r - 1), (3 + 2 * h, 2 * cc + r - 1))
                    for m in range(8):
                        slot = (0, 0, 1, 1, 1, 1, 3, 3)[m]
                        if slot not in slots:
                            continue
                        (k0, g0), (k1, g1) = parts
                        best = jnp.max(jnp.maximum(tops[m, k0, g0], tops[m, k1, g1]), axis=0, keepdims=True)
                        if slot == 1:
                            for i in range(2):
                                pooled[1 + i, cc, pl.ds(row, 1), 256 * (m - 2):256 * (m - 1)] = best[:, 256 * i:256 * i + 256]
                        else:
                            pooled[slot, cc, pl.ds(row, 1), PIECE * (m % 2):PIECE * (m % 2) + PIECE] = best

    def swap(slot):
        for cc in range(2):
            if (slot, cc) != (0, 0):
                send(("e", slot, cc), pooled.at[slot, cc], landed.at[cc, back[slot]], device(dx=DELTA[slot], flip=cc))

    def early():
        pool((0, 1))
        for slot in (1, 2, 0):
            swap(slot)

    acts = {
        "own_s": send_own_s, "own_w": send_own_w, "pair": pair_s, "rows": paired_s, "far": fwd_s,
        "share": share_w, "relay": relay_w, "columns": ready_w, "across": fwd_w, "codes": find_codes, "early": early,
    }

    def handle(todo):
        for name, *values in todo:
            acts[name](*values)

    def multiply(k, m):
        d = jnp.dot(states[k], weights[m], preferred_element_type=jnp.float32)
        tops[m, k] = jnp.max(d.reshape(4, 16, 8, PIECE), axis=1)

    def straight(table):
        for todo, pairs in table:
            handle(todo)
            for k, m in pairs:
                multiply(k, m)

    def looped(table):
        def step(n, _):
            for at, (todo, _) in enumerate(table):
                pl.when(n == at)(lambda: handle(todo))
            for part in range(len(table[0][1])):
                k, m = (
                    sum(jnp.where(n == at, pairs[part][i], 0) for at, (_, pairs) in enumerate(table) if pairs[part][i])
                    for i in range(2)
                )
                multiply(k, m)
            return 0

        lax.fori_loop(0, len(table), step, 0)

    straight(FIRST)
    looped(FOURS)
    looped(EIGHTS)
    straight(LAST)
    pool((3,))
    swap(3)
    landed[0, 0] = pooled[0, 0]

    def leave(name, region):
        copy(name, region, region, device(flip=1)).wait_send()

    leave(("z", 0), states.at[pl.ds(0, 7)])
    by_core(0, lambda first, width: leave(("x", 0, 0), weights.at[pl.ds(0, 3), :, pl.ds(0, width)]))
    leave(("x", 0, 1), weights.at[pl.ds(0, 6), :, pl.ds(0, 384)])
    bias = vbias_ref[...].astype(jnp.float32).reshape(1, -1)
    columns = BLOCK * v + lax.broadcasted_iota(jnp.int32, (8, BLOCK), 1)
    for slot in (0, 1, 2, 3):
        for cc in range(2):
            if (slot, cc) != (0, 0):
                got(("e", back[slot], cc), landed.at[cc, slot])
        raw = jnp.concatenate([landed[c, slot], landed[1 - c, slot][:, 2 * WIDE - BLOCK:]], axis=1) + bias
        done = jnp.where(columns < VOCAB, jnp.log1p(jnp.maximum(raw, 0.0)), 0.0)
        vec[pl.ds(pl.multiple_of(8 * ((x + DELTA[slot] + 4) % 4), 8), 8), :] = done

    for slot in range(LIMIT):
        low = lows[slot:slot + 1, :]
        weight = jnp.zeros((32, LANES), jnp.float32)
        for j in range(15):
            hit = (codes[j] == low) & (low < BIG)
            weight = weight + jnp.where(hit, vec[:, j * LANES:(j + 1) * LANES], 0.0)
        sheet[slot:slot + 1, :] = jnp.sum(weight, axis=0, keepdims=True)
    store = pltpu.make_async_copy(vec, out_ref, local_sem.at[4])
    store.start()
    boxes[...] = jnp.transpose(sheet[...]).reshape(8, 16, LANES)
    for d in range(1, 8):
        to = (b + d) % 8
        send(("pb",), boxes.at[to], batch_in.at[b], (to, v))
    batch_in[b] = boxes[b]
    got(("pb",), batch_in.at[pl.ds(0, 7)])
    for origin in range(8):
        vocab_out[:, origin, :] = batch_in[origin]
    for d in range(1, 16):
        to = (v + d) % 16
        send(("pv",), vocab_out.at[to], sheet_out_ref.at[v], (b, to))
    keep = pltpu.make_async_copy(vocab_out.at[v], sheet_out_ref.at[v], local_sem.at[5])
    keep.start()
    got(("pv",), sheet_out_ref.at[pl.ds(0, 15)])

    store.wait()
    keep.wait()
    leave(("e", 0, 1), tops.at[0, pl.ds(0, 7), pl.ds(0, 2)])
    leave(("pb",), boxes.at[pl.ds(0, 7)])
    leave(("pv",), vocab_out.at[pl.ds(0, 15)])


MESSAGES = 54


def encode(hidden, dense_w, dense_b, norm_gain, norm_bias, vocabulary_weight, vocabulary_bias, lengths, term_ids):
    anywhere = pl.BlockSpec(memory_space=pl.ANY)
    vmem = pl.BlockSpec(memory_space=pltpu.VMEM)
    smem = pl.BlockSpec(memory_space=pltpu.SMEM)
    return pl.pallas_call(
        encode_kernel,
        in_specs=[smem, anywhere, anywhere, vmem, vmem, vmem, anywhere, vmem, anywhere],
        out_specs=[anywhere, anywhere],
        out_shape=[
            jax.ShapeDtypeStruct((32, BLOCK), jnp.float32),
            jax.ShapeDtypeStruct((16, 8, LANES), jnp.float32),
        ],
        scratch_shapes=[
            pltpu.VMEM((512, 768), jnp.bfloat16),
            pltpu.VMEM((768, 768), jnp.bfloat16),
            pltpu.VMEM((8, 512, 768), jnp.bfloat16),
            pltpu.VMEM((8, 768, PIECE), jnp.bfloat16),
            pltpu.VMEM((8, 8, 4, 8, PIECE), jnp.float32),
            pltpu.VMEM((4, 2, 8, WIDE), jnp.float32),
            pltpu.VMEM((2, 4, 8, WIDE), jnp.float32),
            pltpu.VMEM((16, 32, LANES), jnp.int32),
            pltpu.VMEM((8, LANES), jnp.int32),
            pltpu.VMEM((LANES, LANES), jnp.float32),
            pltpu.VMEM((8, 16, LANES), jnp.float32),
            pltpu.VMEM((8, 16, LANES), jnp.float32),
            pltpu.VMEM((16, 8, LANES), jnp.float32),
            pltpu.VMEM((32, BLOCK), jnp.float32),
            pltpu.VMEM((32, K), jnp.int32),
            pltpu.SemaphoreType.DMA((7,)),
            pltpu.SemaphoreType.DMA((6,)),
            pltpu.SemaphoreType.DMA((MESSAGES,)),
        ],
        compiler_params=pltpu.CompilerParams(collective_id=0, has_side_effects=True, vmem_limit_bytes=56 * 2**20),
    )(lengths, hidden, dense_w, dense_b, norm_gain, norm_bias, vocabulary_weight, vocabulary_bias, term_ids)


def finish_kernel(vectors_ref, sheet_ref, out_ref, out_w_ref, out_k_ref, rows):
    out_ref[...] = vectors_ref[...]
    for origin in range(16):
        rows[:, origin, :] = sheet_ref[origin]
    result = jnp.transpose(rows[...].reshape(LANES, LANES))
    out_w_ref[:, 0, :] = result[0:LIMIT]
    out_k_ref[:, 0, :] = result[8:8 + LIMIT].astype(jnp.int32)


def finish(vectors, sheet):
    vmem = pl.BlockSpec(memory_space=pltpu.VMEM)
    return pl.pallas_call(
        finish_kernel,
        in_specs=[vmem, vmem],
        out_specs=[vmem, vmem, vmem],
        out_shape=[
            jax.ShapeDtypeStruct(vectors.shape, jnp.float32),
            jax.ShapeDtypeStruct((LIMIT, 1, LANES), jnp.float32),
            jax.ShapeDtypeStruct((LIMIT, 1, LANES), jnp.int32),
        ],
        scratch_shapes=[pltpu.VMEM((8, 16, LANES), jnp.float32)],
    )(vectors, sheet)


def local(hidden, dense_w, dense_b, norm_gain, norm_bias, vocabulary_weight, vocabulary_bias, lengths, term_ids):
    vectors, sheet = encode(
        hidden, dense_w, dense_b, norm_gain, norm_bias, vocabulary_weight, vocabulary_bias, lengths, term_ids
    )
    vectors, weights, keys = finish(vectors, sheet)
    return vectors, jnp.swapaxes(weights, 0, 1), jnp.swapaxes(keys, 0, 1)


def solution(mesh):
    in_specs = (
        P(("batch", "vocab"), None), P(), P(), P(), P(),
        P(None, "vocab"), P("vocab"), P("batch"), P("batch", None),
    )
    out_specs = (P("batch", "vocab"), P(("batch", "vocab"), None, None), P(("batch", "vocab"), None, None))
    return jax.shard_map(local, mesh=mesh, in_specs=in_specs, out_specs=out_specs, check_vma=False)
```
